32 devices in a mesh: dp: 4 (over y, x), row: 2 (over core), col: 4 (over z).
Axes of the slice: x: 2, y: 2, z: 4, core: 2. Of those that a mesh axis runs over, the one named last changes fastest.
Arguments:
- hidden_state_input: bfloat16 [2048, 1024], P('dp', 'col'), may hold values from -6 to 6
- initial_token_embedding: bfloat16 [2048, 1024], P('dp', 'col'), may hold values from -6 to 6
- document_numbers: int32 [2048], P('dp'), may hold values from 0 to 3, as said below
- document_start_flags: int32 [2048], P('dp'), may hold values from 0 to 1, as said below
- attention_norm_gain: float32 [2, 1024], P(None, 'col'), may hold values from 0.5 to 1.5
- query_key_value_matrix: bfloat16 [3, 2, 1024, 2048], P(None, None, 'col', 'row'), may hold values from -0.125 to 0.125
- attention_out_matrix: bfloat16 [2048, 2, 1024], P('row', None, 'col'), may hold values from -1 to 1
- perceptron_norm_gain: float32 [2, 1024], P(None, 'col'), may hold values from 0.5 to 1.5
- gate_up_matrix: bfloat16 [2, 2, 1024, 4096], P(None, None, 'col', 'row'), may hold values from -0.125 to 0.125
- adapter_down: bfloat16 [2, 1024, 128], P(None, 'col'), may hold values from -0.125 to 0.125
- adapter_up: bfloat16 [2, 128, 4096], P(None, None, ('row', 'col')), may hold values from -0.25 to 0.25
- down_matrix: bfloat16 [4096, 2, 1024], P('row', None, 'col'), may hold values from -0.09375 to 0.09375
- projection_matrix: bfloat16 [2, 1024, 1024], P(None, 'col'), may hold values from -0.125 to 0.125
- mixer_norm_gain: float32 [1024], P('col'), may hold values from 0.5 to 1.5
- gate_in_matrix: bfloat16 [2, 1024, 2048], P(None, 'col', 'row'), may hold values from -0.1875 to 0.1875
- state_in_matrix: bfloat16 [1024, 160], P('col'), may hold values from -0.1875 to 0.1875
- mixer_input_kernel: float32 [4, 2048], P(None, ('row', 'col')), may hold values from -3 to 3
- state_conv_kernel: float32 [4, 128], replicated, may hold values from -3 to 3
- step_offset_bias: float32 [32], P(('row', 'col')), may hold values from -4 to -1
- log_decay_rates: float32 [32], P(('row', 'col')), may hold values from 0 to 2.5
- head_skip_term: float32 [32], P(('row', 'col')), may hold values from 0.5 to 1.5
- gated_norm_gain: float32 [2048], P(('row', 'col')), may hold values from 0.5 to 1.5
- mixer_out_matrix: bfloat16 [2048, 1024], P('row', 'col'), may hold values from -0.125 to 0.125
- output_gradient: bfloat16 [2048, 1024], P('dp', 'col'), may hold values from -6 to 6
Outputs:
- block_out: bfloat16 [2048, 1024], P('dp', 'col')
- grad_hidden: float32 [2048, 1024], P('dp', 'col')
- grad_embed: float32 [2048, 1024], P('dp', 'col')
- grad_gain_attn: float32 [2, 1024], P(None, 'col')
- grad_qkv: float32 [3, 2, 1024, 2048], P(None, None, 'col', 'row')
- grad_attn_out: float32 [2048, 2, 1024], P('row', None, 'col')
- grad_gain_mlp: float32 [2, 1024], P(None, 'col')
- grad_gate_up: float32 [2, 2, 1024, 4096], P(None, None, 'col', 'row')
- grad_lora_down: float32 [2, 1024, 128], P(None, 'col')
- grad_lora_up: float32 [2, 128, 4096], P(None, None, ('row', 'col'))
- grad_down: float32 [4096, 2, 1024], P('row', None, 'col')
- grad_proj: float32 [2, 1024, 1024], P(None, 'col')
- grad_gain_mixer: float32 [1024], P('col')
- grad_in_zx: float32 [2, 1024, 2048], P(None, 'col', 'row')
- grad_in_bcdt: float32 [1024, 160], P('col')
- grad_conv_inner: float32 [4, 2048], P(None, ('row', 'col'))
- grad_conv_state: float32 [4, 128], replicated
- grad_step_bias: float32 [32], P(('row', 'col'))
- grad_decay_log: float32 [32], P(('row', 'col'))
- grad_skip_gain: float32 [32], P(('row', 'col'))
- grad_gain_gated: float32 [2048], P(('row', 'col'))
- grad_out_weight: float32 [2048, 1024], P('row', 'col')
The draws below stay inside these ranges and needn't reach their ends.
Inputs may be any that keep to these rules, and one draw needn't show every extreme that they name: `document_numbers`: each sequence of 512 tokens holds exactly four documents: the id is 0 at the first token and rises by one exactly where document_start_flags is 1. `document_start_flags`: 1 at the first token of every sequence of 512 tokens and where document_numbers rises, four times in each sequence.
All inputs are finite; a program needn't handle non-finite values.
Results may differ from the reference program's by a relative error of at most 0.03.
Values may be sent and summed in bfloat16 or wider, within the bound.
A program may use at most 192 MiB of HBM per device.

```python
import functools
import math
import jax
import jax.numpy as jnp
from jax import lax

MODEL_WIDTH = 1024
CONCAT_WIDTH = 2048
H = 16
HD = 128
HH = 2048
HIDDEN_COUNT = 4096
ADAPTER_RANK = 128
NH = 32
DI = 2048
NS = 64
KW = 4
SEQ_LEN = 512
TOKENS = 2048


def document_starts(key):
    seq_count = TOKENS // SEQ_LEN
    folded = jax.random.fold_in(key, 7)
    seq_keys = jax.random.split(folded, seq_count)
    chosen = jax.vmap(lambda one_key: jax.random.permutation(one_key, SEQ_LEN - 1)[:3])(seq_keys) + 1
    rows = jnp.broadcast_to(jnp.arange(seq_count)[:, None], chosen.shape)
    starts = jnp.zeros((seq_count, SEQ_LEN), jnp.int32)
    starts = starts.at[rows, chosen].set(1)
    starts = starts.at[:, 0].set(1)
    return starts


def draw_document_numbers(key, part):
    starts = document_starts(key)
    return (jnp.cumsum(starts, 1) - 1).astype(jnp.int32).reshape(-1)


def draw_document_start_flags(key, part):
    return document_starts(key).reshape(-1)


def steps_of(stream_key, shape, shards, low, high):
    def one(dim, shards_of):
        steps = jax.random.uniform(jax.random.fold_in(jax.random.fold_in(stream_key, 6), dim), (shards_of,), jnp.float32, low / len(shards), high / len(shards))
        return jnp.repeat(jnp.exp(steps), shape[dim] // shards_of).reshape((-1,) + (1,) * (len(shape) - dim - 1))

    level = one(*shards[0])
    for cut in shards[1:]:
        level = level * one(*cut)
    return level


def noise(stream_key, shape, spread, most, shards=(), kind=jnp.bfloat16):
    result = spread * jax.random.normal(stream_key, shape, jnp.float32)
    if shards:
        result = result * steps_of(stream_key, shape, shards, -0.22, 0.18)
    return jnp.clip(result, -most, most).astype(kind)


def setup_inputs(seed: int = 0) -> dict:
    splits = jax.random.split(jax.random.key(seed), 25)
    return {
        "hidden_state_input": noise(splits[0], (TOKENS, MODEL_WIDTH), 1.0, 6.0, ((0, 4), (1, 4))),
        "initial_token_embedding": noise(splits[1], (TOKENS, MODEL_WIDTH), 1.0, 6.0, ((0, 4), (1, 4))),
        "document_numbers": draw_document_numbers(jax.random.fold_in(splits[24], 71), 0),
        "document_start_flags": draw_document_start_flags(jax.random.fold_in(splits[24], 71), 0),
        "attention_norm_gain": jnp.clip(1.0 + 0.1 * jax.random.normal(splits[4], (2, MODEL_WIDTH), jnp.float32), 0.5, 1.5),
        "query_key_value_matrix": noise(splits[5], (3, 2, MODEL_WIDTH, HH), CONCAT_WIDTH ** -0.5, 0.125, ((2, 4), (3, 2))),
        "attention_out_matrix": noise(splits[6], (HH, 2, MODEL_WIDTH), (HH // 64) ** -0.5, 1.0, ((0, 2), (2, 4))),
        "perceptron_norm_gain": jnp.clip(1.0 + 0.1 * jax.random.normal(splits[7], (2, MODEL_WIDTH), jnp.float32), 0.5, 1.5),
        "gate_up_matrix": noise(splits[8], (2, 2, MODEL_WIDTH, HIDDEN_COUNT), CONCAT_WIDTH ** -0.5, 0.125, ((2, 4), (3, 2))),
        "adapter_down": noise(splits[9], (2, MODEL_WIDTH, ADAPTER_RANK), CONCAT_WIDTH ** -0.5, 0.125, ((1, 4),)),
        "adapter_up": noise(splits[10], (2, ADAPTER_RANK, HIDDEN_COUNT), (4 * ADAPTER_RANK) ** -0.5, 0.25, ((2, 8),)),
        "down_matrix": noise(splits[11], (HIDDEN_COUNT, 2, MODEL_WIDTH), HIDDEN_COUNT ** -0.5, 0.09375, ((0, 2), (2, 4))),
        "projection_matrix": noise(splits[12], (2, MODEL_WIDTH, MODEL_WIDTH), CONCAT_WIDTH ** -0.5, 0.125, ((1, 4),)),
        "mixer_norm_gain": jnp.clip(1.0 + 0.1 * jax.random.normal(splits[13], (MODEL_WIDTH,), jnp.float32), 0.5, 1.5),
        "gate_in_matrix": noise(splits[14], (2, MODEL_WIDTH, DI), MODEL_WIDTH ** -0.5, 0.1875, ((1, 4), (2, 2))),
        "state_in_matrix": noise(splits[15], (MODEL_WIDTH, 2 * NS + NH), MODEL_WIDTH ** -0.5, 0.1875, ((0, 4),)),
        "mixer_input_kernel": noise(splits[16], (KW, DI), 0.5, 3.0, ((1, 8),), jnp.float32),
        "state_conv_kernel": noise(splits[17], (KW, 2 * NS), 0.5, 3.0, (), jnp.float32),
        "step_offset_bias": jnp.clip(-4.0 + 3.0 * jax.random.uniform(splits[18], (NH,), jnp.float32) ** steps_of(splits[18], (NH,), ((0, 8),), -0.2, 0.2), -4.0, -1.0),
        "log_decay_rates": jnp.clip(2.5 * jax.random.uniform(splits[19], (NH,), jnp.float32) ** steps_of(splits[19], (NH,), ((0, 8),), -0.2, 0.2), 0.0, 2.5),
        "head_skip_term": jnp.clip(0.5 + 1.0 * jax.random.uniform(splits[20], (NH,), jnp.float32) ** steps_of(splits[20], (NH,), ((0, 8),), -0.2, 0.2), 0.5, 1.5),
        "gated_norm_gain": jnp.clip(1.0 + 0.1 * jax.random.normal(splits[21], (DI,), jnp.float32), 0.5, 1.5),
        "mixer_out_matrix": noise(splits[22], (DI, MODEL_WIDTH), DI ** -0.5, 0.125, ((0, 2), (1, 4))),
        "output_gradient": noise(splits[23], (TOKENS, MODEL_WIDTH), 1.0, 6.0, ((0, 4), (1, 4))),
    }


EPS = 1e-05
FULL_PRECISION = lax.Precision.HIGHEST

def matrix_product(left, right):
    return jnp.dot(left, right, preferred_element_type=jnp.float32)

def matmul_tn(left, right):
    return lax.dot_general(left, right, (((0,), (0,)), ((), ())), preferred_element_type=jnp.float32)

def matrix_product_transposed(left, right):
    return lax.dot_general(left, right, (((1,), (1,)), ((), ())), preferred_element_type=jnp.float32)

def exact_product(left, right):
    return jnp.dot(left, right, precision=FULL_PRECISION)

def rope_tables(length, width):
    half = width // 2
    positions = jnp.arange(length).astype(jnp.float32)
    rates = jnp.exp(-math.log(10000.0) * jnp.arange(half).astype(jnp.float32) / half)
    angles = positions[:, None] * rates[None, :]
    return (jnp.cos(angles)[:, None, :], jnp.sin(angles)[:, None, :])

def rotate(vectors, cosine, sine):
    half = vectors.shape[-1] // 2
    first = vectors[..., :half]
    second = vectors[..., half:]
    return jnp.concatenate([first * cosine - second * sine, first * sine + second * cosine], -1)

def attention_core(queries, keys, values, segment):
    length = queries.shape[0]
    width = queries.shape[2]
    cosine, sine = rope_tables(length, width)
    queries = rotate(queries, cosine, sine)
    keys = rotate(keys, cosine, sine)
    scores = jnp.einsum('qhd,khd->hqk', queries, keys, precision=FULL_PRECISION) / math.sqrt(width)
    places = jnp.arange(length)
    allowed = (places[:, None] >= places[None, :]) & (segment[:, None] == segment[None, :])
    weight_list = jnp.where(allowed[None], jnp.exp(scores), 0.0)
    weight_list = weight_list / lax.optimization_barrier(jnp.sum(weight_list, -1, keepdims=True))
    return jnp.einsum('hqk,khd->qhd', weight_list, values, precision=FULL_PRECISION)

def conv_causal(signal, kernel, docs):
    total = signal * kernel[0]
    for offset in range(1, kernel.shape[0]):
        shifted = jnp.concatenate([jnp.zeros((offset, signal.shape[1]), signal.dtype), signal[:-offset]], 0)
        shifted_docs = jnp.concatenate([jnp.full((offset,), -1, jnp.int32), docs[:-offset]], 0)
        same = (shifted_docs == docs).astype(signal.dtype)[:, None]
        total = total + shifted * kernel[offset] * same
    return total

def bc_activate(bc_pre, kernel, docs):
    return jax.nn.silu(conv_causal(bc_pre, kernel, docs))

def mixer_core(x_pre, gate_z, step_raw, bc_conv, conv_kernel, step_offset_bias, log_decay_rates, head_skip_term, docs):
    length = x_pre.shape[0]
    heads = step_raw.shape[1]
    head_dim = x_pre.shape[1] // heads
    state = bc_conv.shape[1] // 2
    inner = jax.nn.silu(conv_causal(x_pre, conv_kernel, docs)).reshape(length, heads, head_dim)
    b_states = bc_conv[:, :state]
    c_states = bc_conv[:, state:]
    step = jax.nn.softplus(step_raw + step_offset_bias)
    rate = -jnp.exp(log_decay_rates) * step
    cumulative = jnp.cumsum(rate, 0)
    places = jnp.arange(length)
    allowed = ((places[:, None] >= places[None, :]) & (docs[:, None] == docs[None, :]))[None]
    gaps = cumulative.T[:, :, None] - cumulative.T[:, None, :]
    decay = jnp.where(allowed, jnp.exp(jnp.where(allowed, gaps, 0.0)), 0.0)
    intersection = jnp.dot(c_states, b_states.T, precision=FULL_PRECISION)
    mixing = decay * intersection[None]
    weighted = inner * step[:, :, None]
    outputs = jnp.einsum('hts,shp->thp', mixing, weighted, precision=FULL_PRECISION)
    outputs = outputs + head_skip_term[None, :, None] * inner
    return outputs.reshape(length, heads * head_dim) * jax.nn.silu(gate_z)

def gelu_product(gate_preact, up_preact):
    return jax.nn.gelu(gate_preact, approximate=True) * up_preact

def rms_forward(values):
    scale = lax.rsqrt(lax.optimization_barrier(jnp.mean(values * values, -1, keepdims=True)) + EPS)
    return (values * scale, scale)

def rms_backward(grad_in, normal, scale, gain):
    grad_hat = grad_in * gain
    inner = lax.optimization_barrier(jnp.mean(grad_hat * normal, -1, keepdims=True))
    return (scale * (grad_hat - normal * inner), lax.optimization_barrier(jnp.sum(grad_in * normal, 0)))

def one_sequence(weight_list, hidden, embed, segment, resets, cotangent):
    attention_norm_gain, query_key_value_matrix, attention_out_matrix, perceptron_norm_gain, gate_up_matrix, adapter_down, adapter_up, down_matrix, projection_matrix, mixer_norm_gain, gate_in_matrix, state_in_matrix, mixer_input_kernel, state_conv_kernel, step_offset_bias, log_decay_rates, head_skip_term, gated_norm_gain, mixer_out_matrix = weight_list
    length = hidden.shape[0]
    qkv_flat = query_key_value_matrix.reshape(3, CONCAT_WIDTH, HH)
    attn_out_flat = attention_out_matrix.reshape(HH, CONCAT_WIDTH)
    gate_up_rows = gate_up_matrix.reshape(2, CONCAT_WIDTH, HIDDEN_COUNT)
    adapter_down_rows = adapter_down.reshape(CONCAT_WIDTH, ADAPTER_RANK)
    adapter_up_broad = adapter_up.astype(jnp.float32)
    down_flat = down_matrix.reshape(HIDDEN_COUNT, CONCAT_WIDTH)
    proj_flat = projection_matrix.reshape(CONCAT_WIDTH, MODEL_WIDTH)
    attn_gain = attention_norm_gain.reshape(CONCAT_WIDTH)
    mlp_gain = perceptron_norm_gain.reshape(CONCAT_WIDTH)
    concat = jnp.concatenate([hidden, embed], 1).astype(jnp.float32)
    norm_one, scale_one = rms_forward(concat)
    normed_one = (norm_one * attn_gain).astype(jnp.bfloat16)
    queries = matrix_product(normed_one, qkv_flat[0]).reshape(length, H, HD)
    keys_pre = matrix_product(normed_one, qkv_flat[1]).reshape(length, H, HD)
    values_pre = matrix_product(normed_one, qkv_flat[2]).reshape(length, H, HD)
    attended = attention_core(queries, keys_pre, values_pre, segment)
    heads_out = attended.reshape(length, HH).astype(jnp.bfloat16)
    attn_stream = concat + matrix_product(heads_out, attn_out_flat)
    norm_two, scale_two = rms_forward(attn_stream)
    second_normed = (norm_two * mlp_gain).astype(jnp.bfloat16)
    adapter_middle = matrix_product(second_normed, adapter_down_rows)
    gate_preact = matrix_product(second_normed, gate_up_rows[0]) + exact_product(adapter_middle, adapter_up_broad[0])
    up_preact = matrix_product(second_normed, gate_up_rows[1]) + exact_product(adapter_middle, adapter_up_broad[1])
    hidden_units = gelu_product(gate_preact, up_preact).astype(jnp.bfloat16)
    mixed = attn_stream + matrix_product(hidden_units, down_flat)
    mixed_b = mixed.astype(jnp.bfloat16)
    resid = hidden.astype(jnp.float32) + matrix_product(mixed_b, proj_flat)
    norm_three, scale_three = rms_forward(resid)
    normed_three = (norm_three * mixer_norm_gain).astype(jnp.bfloat16)
    gate_z = matrix_product(normed_three, gate_in_matrix[0])
    x_pre = matrix_product(normed_three, gate_in_matrix[1])
    bcdt = matrix_product(normed_three, state_in_matrix)
    state_cols = 2 * NS
    docs = (jnp.cumsum(resets) - 1).astype(jnp.int32)
    bc_conv = bc_activate(bcdt[:, :state_cols], state_conv_kernel, docs)
    gated = mixer_core(x_pre, gate_z, bcdt[:, state_cols:], bc_conv, mixer_input_kernel, step_offset_bias, log_decay_rates, head_skip_term, docs)
    norm_four, scale_four = rms_forward(gated)
    normed_four = (norm_four * gated_norm_gain).astype(jnp.bfloat16)
    output = resid + matrix_product(normed_four, mixer_out_matrix)
    block_out = output.astype(jnp.bfloat16)
    grad_top = cotangent.astype(jnp.float32)
    grad_mixer_out_matrix = matmul_tn(normed_four, cotangent)
    d_normed_four = matrix_product_transposed(cotangent, mixer_out_matrix)
    d_gated, grad_gated_gain = rms_backward(d_normed_four, norm_four, scale_four, gated_norm_gain)
    core_back = jax.vjp(functools.partial(mixer_core, docs=docs), x_pre, gate_z, bcdt[:, state_cols:], bc_conv, mixer_input_kernel, step_offset_bias, log_decay_rates, head_skip_term)[1]
    d_x_pre, d_gate_z, d_step_raw, d_bc_conv, grad_mixer_input_kernel, grad_step_offset_bias, grad_log_decay, grad_head_skip = core_back(d_gated)
    bc_back = jax.vjp(functools.partial(bc_activate, docs=docs), bcdt[:, :state_cols], state_conv_kernel)[1]
    d_bc_pre, grad_state_conv_kernel = bc_back(d_bc_conv)
    d_bcdt_b = jnp.concatenate([d_bc_pre, d_step_raw], 1).astype(jnp.bfloat16)
    d_zx_b = jnp.stack([d_gate_z, d_x_pre]).astype(jnp.bfloat16)
    grad_gate_in_matrix = jnp.stack([matmul_tn(normed_three, d_zx_b[0]), matmul_tn(normed_three, d_zx_b[1])])
    grad_state_in_matrix = matmul_tn(normed_three, d_bcdt_b)
    d_normed_three = matrix_product_transposed(d_zx_b[0], gate_in_matrix[0]) + matrix_product_transposed(d_zx_b[1], gate_in_matrix[1]) + matrix_product_transposed(d_bcdt_b, state_in_matrix)
    d_norm_three, grad_mixer_gain = rms_backward(d_normed_three, norm_three, scale_three, mixer_norm_gain)
    d_resid = grad_top + d_norm_three
    d_resid_b = d_resid.astype(jnp.bfloat16)
    grad_projection_matrix = matmul_tn(mixed_b, d_resid_b).reshape(2, MODEL_WIDTH, MODEL_WIDTH)
    d_mixed = matrix_product_transposed(d_resid_b, proj_flat)
    d_mixed_b = d_mixed.astype(jnp.bfloat16)
    grad_down_matrix = matmul_tn(hidden_units, d_mixed_b).reshape(HIDDEN_COUNT, 2, MODEL_WIDTH)
    d_hidden_units = matrix_product_transposed(d_mixed_b, down_flat)
    act_back = jax.vjp(gelu_product, gate_preact, up_preact)[1]
    grad_gate_preact, grad_up_preact = act_back(d_hidden_units)
    grad_adapter_up = jnp.stack([exact_product(adapter_middle.T, grad_gate_preact), exact_product(adapter_middle.T, grad_up_preact)])
    grad_adapter_middle = exact_product(grad_gate_preact, adapter_up_broad[0].T) + exact_product(grad_up_preact, adapter_up_broad[1].T)
    grad_gate_block = grad_gate_preact.astype(jnp.bfloat16)
    grad_up_block = grad_up_preact.astype(jnp.bfloat16)
    grad_gate_up_matrix = jnp.stack([matmul_tn(second_normed, grad_gate_block), matmul_tn(second_normed, grad_up_block)]).reshape(2, 2, MODEL_WIDTH, HIDDEN_COUNT)
    grad_second_normed = matrix_product_transposed(grad_gate_block, gate_up_rows[0]) + matrix_product_transposed(grad_up_block, gate_up_rows[1]) + exact_product(grad_adapter_middle, adapter_down_rows.astype(jnp.float32).T)
    grad_adapter_down = exact_product(second_normed.astype(jnp.float32).T, grad_adapter_middle).reshape(2, MODEL_WIDTH, ADAPTER_RANK)
    d_norm_two, grad_perceptron_gain = rms_backward(grad_second_normed, norm_two, scale_two, mlp_gain)
    d_attn = d_mixed + d_norm_two
    d_attn_b = d_attn.astype(jnp.bfloat16)
    grad_attention_out = matmul_tn(heads_out, d_attn_b).reshape(HH, 2, MODEL_WIDTH)
    d_heads = matrix_product_transposed(d_attn_b, attn_out_flat).reshape(length, H, HD)
    attn_back = jax.vjp(functools.partial(attention_core, segment=segment), queries, keys_pre, values_pre)[1]
    d_queries, d_keys, d_values = attn_back(d_heads)
    d_qkv_b = jnp.stack([d_queries, d_keys, d_values]).reshape(3, length, HH).astype(jnp.bfloat16)
    grad_query_key_value = jnp.stack([matmul_tn(normed_one, d_qkv_b[0]), matmul_tn(normed_one, d_qkv_b[1]), matmul_tn(normed_one, d_qkv_b[2])]).reshape(3, 2, MODEL_WIDTH, HH)
    d_normed_one = matrix_product_transposed(d_qkv_b[0], qkv_flat[0]) + matrix_product_transposed(d_qkv_b[1], qkv_flat[1]) + matrix_product_transposed(d_qkv_b[2], qkv_flat[2])
    d_norm_one, grad_attention_gain = rms_backward(d_normed_one, norm_one, scale_one, attn_gain)
    d_concat = d_attn + d_norm_one
    grad_hidden = d_resid + d_concat[:, :MODEL_WIDTH]
    grad_embed = d_concat[:, MODEL_WIDTH:]
    gradient_list = (grad_attention_gain.reshape(2, MODEL_WIDTH), grad_query_key_value, grad_attention_out, grad_perceptron_gain.reshape(2, MODEL_WIDTH), grad_gate_up_matrix, grad_adapter_down, grad_adapter_up, grad_down_matrix, grad_projection_matrix, grad_mixer_gain, grad_gate_in_matrix, grad_state_in_matrix, grad_mixer_input_kernel, grad_state_conv_kernel, grad_step_offset_bias, grad_log_decay, grad_head_skip, grad_gated_gain, grad_mixer_out_matrix)
    return ((block_out, grad_hidden, grad_embed), gradient_list)

def reference(hidden_state_input, initial_token_embedding, document_numbers, document_start_flags, attention_norm_gain, query_key_value_matrix, attention_out_matrix, perceptron_norm_gain, gate_up_matrix, adapter_down, adapter_up, down_matrix, projection_matrix, mixer_norm_gain, gate_in_matrix, state_in_matrix, mixer_input_kernel, state_conv_kernel, step_offset_bias, log_decay_rates, head_skip_term, gated_norm_gain, mixer_out_matrix, output_gradient):
    weight_list = (attention_norm_gain, query_key_value_matrix, attention_out_matrix, perceptron_norm_gain, gate_up_matrix, adapter_down, adapter_up, down_matrix, projection_matrix, mixer_norm_gain, gate_in_matrix, state_in_matrix, mixer_input_kernel, state_conv_kernel, step_offset_bias, log_decay_rates, head_skip_term, gated_norm_gain, mixer_out_matrix)
    seq_count = hidden_state_input.shape[0] // SEQ_LEN
    pieces = (hidden_state_input.reshape(seq_count, SEQ_LEN, MODEL_WIDTH), initial_token_embedding.reshape(seq_count, SEQ_LEN, MODEL_WIDTH), document_numbers.reshape(seq_count, SEQ_LEN), document_start_flags.reshape(seq_count, SEQ_LEN), output_gradient.reshape(seq_count, SEQ_LEN, MODEL_WIDTH))

    def fold(totals, piece):
        results, gradient_list = one_sequence(weight_list, piece[0], piece[1], piece[2], piece[3], piece[4])
        return (tuple((left + right for left, right in zip(totals, gradient_list))), results)
    start = tuple((jnp.zeros(weight.shape, jnp.float32) for weight in weight_list))
    totals, results = lax.scan(fold, start, pieces)
    block_out = results[0].reshape(seq_count * SEQ_LEN, MODEL_WIDTH)
    grad_hidden = results[1].reshape(seq_count * SEQ_LEN, MODEL_WIDTH)
    grad_embed = results[2].reshape(seq_count * SEQ_LEN, MODEL_WIDTH)
    return (block_out, grad_hidden, grad_embed, totals[0], totals[1], totals[2], totals[3], totals[4], totals[5], totals[6], totals[7], totals[8], totals[9], totals[10], totals[11], totals[12], totals[13], totals[14], totals[15], totals[16], totals[17], totals[18])
```

```python
import functools
import math

import jax
import jax.numpy as jnp
from jax import lax
from jax.experimental import pallas as pl
from jax.experimental.pallas import tpu as pltpu
from jax.sharding import PartitionSpec as P

EPS = 1e-05
FULL_PRECISION = lax.Precision.HIGHEST
BF = jnp.bfloat16
F32 = jnp.float32
MESH = pl.DeviceIdType.MESH


def matrix_product(left, right):
    return jnp.dot(left, right, preferred_element_type=F32)


def matmul_tn(left, right):
    return lax.dot_general(left, right, (((0,), (0,)), ((), ())), preferred_element_type=F32)


def matrix_product_transposed(left, right):
    return lax.dot_general(left, right, (((1,), (1,)), ((), ())), preferred_element_type=F32)


def rope_tables(length, width):
    half = width // 2
    positions = jnp.arange(length).astype(F32)
    rates = jnp.exp(-math.log(10000.0) * jnp.arange(half).astype(F32) / half)
    angles = positions[:, None] * rates[None, :]
    return (jnp.cos(angles)[:, None, :], jnp.sin(angles)[:, None, :])


def rotate(vectors, cosine, sine):
    half = vectors.shape[-1] // 2
    first = vectors[..., :half]
    second = vectors[..., half:]
    return jnp.concatenate([first * cosine - second * sine, first * sine + second * cosine], -1)


def attention_core(queries, keys, values, segment):
    length = queries.shape[0]
    width = queries.shape[2]
    cosine, sine = rope_tables(length, width)
    queries = rotate(queries, cosine, sine)
    keys = rotate(keys, cosine, sine)
    scores = jnp.einsum("qhd,khd->hqk", queries, keys, precision=FULL_PRECISION) / math.sqrt(width)
    places = jnp.arange(length)
    allowed = (places[:, None] >= places[None, :]) & (segment[:, None] == segment[None, :])
    weight_list = jnp.where(allowed[None], jnp.exp(scores), 0.0)
    weight_list = weight_list / jnp.sum(weight_list, -1, keepdims=True)
    return jnp.einsum("hqk,khd->qhd", weight_list, values, precision=FULL_PRECISION)


def conv_causal(signal, kernel, docs):
    total = signal * kernel[0]
    for offset in range(1, kernel.shape[0]):
        shifted = jnp.concatenate(
            [jnp.zeros((offset, signal.shape[1]), signal.dtype), signal[:-offset]], 0
        )
        shifted_docs = jnp.concatenate([jnp.full((offset,), -1, jnp.int32), docs[:-offset]], 0)
        same = (shifted_docs == docs).astype(signal.dtype)[:, None]
        total = total + shifted * kernel[offset] * same
    return total


def bc_activate(bc_pre, kernel, docs):
    return jax.nn.silu(conv_causal(bc_pre, kernel, docs))


def mixer_core(
    x_pre,
    gate_z,
    step_raw,
    bc_conv,
    conv_kernel,
    step_offset_bias,
    log_decay_rates,
    head_skip_term,
    docs,
):
    length = x_pre.shape[0]
    heads = step_raw.shape[1]
    head_dim = x_pre.shape[1] // heads
    state = bc_conv.shape[1] // 2
    inner = jax.nn.silu(conv_causal(x_pre, conv_kernel, docs)).reshape(length, heads, head_dim)
    b_states = bc_conv[:, :state]
    c_states = bc_conv[:, state:]
    step = jax.nn.softplus(step_raw + step_offset_bias)
    rate = -jnp.exp(log_decay_rates) * step
    cumulative = jnp.cumsum(rate, 0)
    places = jnp.arange(length)
    allowed = ((places[:, None] >= places[None, :]) & (docs[:, None] == docs[None, :]))[None]
    gaps = cumulative.T[:, :, None] - cumulative.T[:, None, :]
    decay = jnp.where(allowed, jnp.exp(jnp.where(allowed, gaps, 0.0)), 0.0)
    intersection = jnp.dot(c_states, b_states.T, precision=FULL_PRECISION)
    mixing = decay * intersection[None]
    weighted = inner * step[:, :, None]
    outputs = jnp.einsum("hts,shp->thp", mixing, weighted, precision=FULL_PRECISION)
    outputs = outputs + head_skip_term[None, :, None] * inner
    return outputs.reshape(length, heads * head_dim) * jax.nn.silu(gate_z)


def gelu_product(gate_preact, up_preact):
    return jax.nn.gelu(gate_preact, approximate=True) * up_preact


def _window(index, size):
    return pl.ds(pl.multiple_of(index * size, size), size)


def _add_rows(rows, write):
    chunk = 64 if rows % 64 == 0 else rows
    if rows == chunk:
        write(pl.ds(0, rows))
        return

    def step(i, carry):
        write(pl.ds(pl.multiple_of(i * chunk, chunk), chunk))
        return carry

    lax.fori_loop(0, rows // chunk, step, 0)


def _remote(src, dst, send, recv, device):
    copy = pltpu.make_async_remote_copy(
        src_ref=src,
        dst_ref=dst,
        send_sem=send,
        recv_sem=recv,
        device_id=device,
        device_id_type=MESH,
    )
    copy.start()
    return copy


class Env:
    def __init__(self, n):
        self.n = n
        self.col = lax.axis_index("col")
        self.row = lax.axis_index("row")
        self.sibling = {"row": 1 - self.row}

    def peer(self, k):
        return {"col": lax.rem(self.col + k, self.n)}


def run_gather(env, x, o, send, recv, local):
    width = x.shape[1]
    here = o.at[:, _window(env.col, width)]
    copies = [
        _remote(x, here, send.at[k - 1], recv.at[k - 1], env.peer(k)) for k in range(1, env.n)
    ]
    own = pltpu.make_async_copy(x, here, local.at[0])
    own.start()
    yield
    own.wait()
    for copy in copies:
        copy.wait()


def run_gather2(env, x, o, send, recv, local, send2, recv2):
    width = x.shape[1]
    half = x.shape[0] // 2
    mine = _window(env.row, half)
    copies = [
        _remote(
            x.at[mine, :],
            o.at[mine, _window(env.col, width)],
            send.at[k - 1],
            recv.at[k - 1],
            env.peer(k),
        )
        for k in range(1, env.n)
    ]
    own = pltpu.make_async_copy(x, o.at[:, _window(env.col, width)], local.at[0])
    own.start()
    yield
    onward = []
    for k in range(1, env.n):
        copies[k - 1].wait()
        part = o.at[mine, _window(lax.rem(env.col + env.n - k, env.n), width)]
        onward.append(_remote(part, part, send2.at[k - 1], recv2.at[k - 1], env.sibling))
    yield
    own.wait()
    for copy in onward:
        copy.wait()


def run_scatter(env, p, o, buffer, send, recv):
    rows, width = o.shape
    copies = [
        _remote(
            p.at[:, _window(lax.rem(env.col + k, env.n), width)],
            buffer.at[k - 1],
            send.at[k - 1],
            recv.at[k - 1],
            env.peer(k),
        )
        for k in range(1, env.n)
    ]
    yield
    for copy in copies:
        copy.wait()

    def write(part):
        total = p[part, _window(env.col, width)].astype(F32)
        for k in range(env.n - 1):
            total = total + buffer[k, part, :].astype(F32)
        o[part, :] = total

    _add_rows(rows, write)


def run_scatter2(env, p, o, buffer, send, recv, send2, recv2):
    rows, width = p.shape[0], o.shape[1]
    copies = [
        _remote(
            p.at[:, _window(lax.rem(env.col + k, env.n), width)],
            buffer.at[k - 1],
            send.at[k - 1],
            recv.at[k - 1],
            env.peer(k),
        )
        for k in range(1, env.n)
    ]
    yield
    for copy in copies:
        copy.wait()
    first = env.row * rows

    def write(part):
        total = p[part, _window(env.col, width)].astype(F32)
        for k in range(env.n - 1):
            total = total + buffer[k, part, :].astype(F32)
        target = pl.ds(pl.multiple_of(first + part.start, 8), part.size)
        o[target, :] = total

    _add_rows(rows, write)
    half = o.at[_window(env.row, rows), :]
    copy = _remote(half, half, send2.at[0], recv2.at[0], env.sibling)
    yield
    copy.wait()


def run_reduce(env, p, o, pairs, sums, buffer, send, recv, send2, recv2, send3, recv3):
    rows, width = o.shape
    half = rows // 2
    mine, other = _window(env.row, half), _window(1 - env.row, half)
    order = [(k + 1) % env.n for k in range(env.n)]
    first = []
    for i, k in enumerate(order):
        piece = _window(lax.rem(env.col + k, env.n), width)
        first.append(
            _remote(p.at[other, piece], pairs.at[i], send.at[i], recv.at[i], env.sibling)
        )
    yield
    start = env.row * half
    copies = []
    for i, k in enumerate(order):
        first[i].wait()
        piece = _window(lax.rem(env.col + k, env.n), width)

        def write(part, i=i, piece=piece, k=k):
            source = pl.ds(pl.multiple_of(start + part.start, 16), part.size)
            total = p[source, piece].astype(F32) + pairs[i, part, :].astype(F32)
            sums[i, part, :] = total.astype(sums.dtype)

        _add_rows(half, write)
        if k:
            copies.append(
                _remote(sums.at[i], buffer.at[i], send2.at[i], recv2.at[i], env.peer(k))
            )
    yield
    for copy in copies:
        copy.wait()

    def finish(part):
        total = sums[env.n - 1, part, :].astype(F32)
        for k in range(env.n - 1):
            total = total + buffer[k, part, :].astype(F32)
        target = pl.ds(pl.multiple_of(start + part.start, 8), part.size)
        o[target, :] = total

    _add_rows(half, finish)
    part = o.at[mine, :]
    copy = _remote(part, part, send3.at[0], recv3.at[0], env.sibling)
    yield
    copy.wait()


def run_a2a(env, x, o, send, recv, local):
    width = o.shape[2]
    copies = [
        _remote(
            x.at[:, _window(lax.rem(env.col + k, env.n), width)],
            o.at[env.col],
            send.at[k - 1],
            recv.at[k - 1],
            env.peer(k),
        )
        for k in range(1, env.n)
    ]
    own = pltpu.make_async_copy(x.at[:, _window(env.col, width)], o.at[env.col], local.at[0])
    own.start()
    yield
    own.wait()
    for copy in copies:
        copy.wait()


def run_a2a_back(env, x, o, send, recv, local):
    width = x.shape[2]
    here = o.at[:, _window(env.col, width)]
    copies = [
        _remote(x.at[lax.rem(env.col + k, env.n)], here, send.at[k - 1], recv.at[k - 1], env.peer(k))
        for k in range(1, env.n)
    ]
    own = pltpu.make_async_copy(x.at[env.col], here, local.at[0])
    own.start()
    yield
    own.wait()
    for copy in copies:
        copy.wait()


def run_rowsum(env, p, o, buffer, send, recv):
    copy = _remote(p, buffer, send.at[0], recv.at[0], env.sibling)
    yield
    copy.wait()

    def write(part):
        o[part, :] = p[part, :].astype(F32) + buffer[part, :].astype(F32)

    _add_rows(p.shape[0], write)


def run_sum(env, s, o, buffer, send, recv, local):
    both = buffer.shape[0] > env.n
    mine = env.row * env.n + env.col if both else env.col
    copies = []
    for r in range(2 if both else 1):
        for k in range(env.n):
            if r == 0 and k == 0:
                continue
            device = dict(env.peer(k)) if k else {}
            if r:
                device["row"] = 1 - env.row
            index = r * env.n + k - 1
            copies.append(_remote(s, buffer.at[mine], send.at[index], recv.at[index], device))
    own = pltpu.make_async_copy(s, buffer.at[mine], local.at[0])
    own.start()
    yield
    own.wait()
    for copy in copies:
        copy.wait()
    total = buffer[0]
    for i in range(1, buffer.shape[0]):
        total = total + buffer[i]
    o[...] = total


def plan(kind, x, n):
    dma = pltpu.SemaphoreType.DMA
    shape = x.shape
    three = dma((n - 1,))
    one = dma((1,))
    if kind == "gather":
        return run_gather, (shape[0], n * shape[1]), x.dtype, [three, three, one]
    if kind == "gather2":
        return run_gather2, (shape[0], n * shape[1]), x.dtype, [three, three, one, three, three]
    if kind == "scatter":
        out = (shape[0], shape[1] // n)
        return run_scatter, out, F32, [pltpu.VMEM((n - 1,) + out, x.dtype), three, three]
    if kind == "scatter2":
        part = (shape[0], shape[1] // n)
        out = (2 * shape[0], shape[1] // n)
        scratch = [pltpu.VMEM((n - 1,) + part, x.dtype), three, three, one, one]
        return run_scatter2, out, F32, scratch
    if kind == "reduce":
        out = (shape[0], shape[1] // n)
        part = (shape[0] // 2, shape[1] // n)
        four = dma((n,))
        scratch = [
            pltpu.VMEM((n,) + part, x.dtype),
            pltpu.VMEM((n,) + part, x.dtype),
            pltpu.VMEM((n - 1,) + part, x.dtype),
            four,
            four,
            three,
            three,
            one,
            one,
        ]
        return run_reduce, out, F32, scratch
    if kind == "a2a":
        return run_a2a, (n, shape[0], shape[1] // n), x.dtype, [three, three, one]
    if kind == "a2a_back":
        return run_a2a_back, (shape[1], n * shape[2]), x.dtype, [three, three, one]
    if kind == "rowsum":
        return run_rowsum, shape, F32, [pltpu.VMEM(shape, x.dtype), one, one]
    members = n if kind == "colsum" else 2 * n
    many = dma((members - 1,))
    return run_sum, shape, F32, [pltpu.VMEM((members,) + shape, x.dtype), many, many, one]


def exchange(ident, items, micros):
    n = lax.axis_size("col")
    plans = [plan(kind, x, n) for kind, x in items]
    kinds = {kind for kind, _ in items}
    count = len(items)
    use_all = "allsum" in kinds
    use_col = use_all or bool(kinds - {"rowsum"})
    use_row = use_all or bool(kinds & {"rowsum", "gather2", "scatter2", "reduce"})

    def kernel(*refs):
        env = Env(n)
        barrier = pltpu.get_barrier_semaphore()
        targets = []
        if use_col:
            targets += [env.peer(k) for k in range(1, n)]
        if use_row:
            targets.append(env.sibling)
        if use_all:
            targets += [{**env.peer(k), **env.sibling} for k in range(1, n)]
        for target in targets:
            pl.semaphore_signal(barrier, inc=1, device_id=target, device_id_type=MESH)
        pl.semaphore_wait(barrier, len(targets))
        position = 2 * count
        running = []
        for i in range(count):
            size = len(plans[i][3])
            scratch = refs[position : position + size]
            position += size
            running.append(plans[i][0](env, refs[i], refs[count + i], *scratch))
        while running:
            alive = []
            for item in running:
                try:
                    next(item)
                except StopIteration:
                    continue
                alive.append(item)
            running = alive

    vmem = pl.BlockSpec(memory_space=pltpu.VMEM)
    return pl.pallas_call(
        kernel,
        out_shape=[jax.ShapeDtypeStruct(p[1], p[2]) for p in plans],
        in_specs=[vmem] * count,
        out_specs=[vmem] * count,
        scratch_shapes=[s for p in plans for s in p[3]],
        compiler_params=pltpu.CompilerParams(collective_id=ident, has_side_effects=True),
        cost_estimate=pl.CostEstimate(
            flops=0, bytes_accessed=int(micros * 3000000), transcendentals=0
        ),
        name="exchange_%d" % ident,
    )(*[x for _, x in items])


def pack_rows(*vectors):
    return jnp.concatenate([v.reshape(-1, 128) for v in vectors], 0)


def unpack_rows(packed, count):
    return [part.reshape(-1) for part in jnp.split(packed, count, 0)]


def body(
    hidden_state_input,
    initial_token_embedding,
    document_numbers,
    document_start_flags,
    attention_norm_gain,
    query_key_value_matrix,
    attention_out_matrix,
    perceptron_norm_gain,
    gate_up_matrix,
    adapter_down,
    adapter_up,
    down_matrix,
    projection_matrix,
    mixer_norm_gain,
    gate_in_matrix,
    state_in_matrix,
    mixer_input_kernel,
    state_conv_kernel,
    step_offset_bias,
    log_decay_rates,
    head_skip_term,
    gated_norm_gain,
    mixer_out_matrix,
    output_gradient,
):
    n = lax.axis_size("col")
    replicas = lax.axis_size("dp")
    dp, row, col = lax.axis_index("dp"), lax.axis_index("row"), lax.axis_index("col")
    length, width = hidden_state_input.shape
    local_width = 2 * width
    model_width = n * width
    concat_width = n * local_width
    inner_width = gated_norm_gain.shape[0] * 2 * n

    def my_rows(weight):
        axis = weight.ndim - 2
        share = weight.shape[axis] // replicas
        part = lax.dynamic_slice_in_dim(weight, dp * share, share, axis)
        return part.reshape(-1, weight.shape[-1])

    def spread(pieces, lead):
        shaped = pieces.reshape(n, lead, -1, pieces.shape[2])
        return lax.all_gather(shaped, "dp", axis=2, tiled=True)

    def features_first(full, outer):
        inner = full.shape[1] // outer
        parts = full.reshape(n, outer, inner * full.shape[2], full.shape[3])
        return parts.transpose(1, 0, 2, 3).reshape(outer, -1, full.shape[3])

    attn_gain = attention_norm_gain.reshape(local_width)
    mlp_gain = perceptron_norm_gain.reshape(local_width)
    attn_out_flat = attention_out_matrix.reshape(attention_out_matrix.shape[0], local_width)
    down_flat = down_matrix.reshape(down_matrix.shape[0], local_width)
    proj_flat = projection_matrix.reshape(local_width, projection_matrix.shape[2])
    adapter_up_broad = adapter_up.astype(F32)
    state_width = state_in_matrix.shape[1]
    state_pad = jnp.pad(state_in_matrix, ((0, 0), (0, -state_width % 128)))

    (qkv_pieces,) = exchange(0, [("a2a", my_rows(query_key_value_matrix))], 20)
    qkv_t = features_first(spread(qkv_pieces, 6), 3)

    concat = (
        jnp.stack([hidden_state_input, initial_token_embedding], 1)
        .astype(F32)
        .reshape(length, local_width)
    )
    x_one, sum_one, gate_up_pieces, gate_in_pieces, adapter_down_full, state_full = exchange(
        1,
        [
            ("gather2", (concat * attn_gain).astype(BF)),
            ("colsum", pack_rows(jnp.sum(concat * concat, 1))),
            ("a2a", my_rows(gate_up_matrix)),
            ("a2a", my_rows(gate_in_matrix)),
            ("gather2", adapter_down.reshape(local_width, -1)),
            ("gather2", state_pad),
        ],
        60,
    )
    gate_up_t = features_first(spread(gate_up_pieces, 4), 2)
    gate_in_t = features_first(spread(gate_in_pieces, 2), 2)

    def stacked(gathered, lanes):
        rows = gathered.shape[0]
        return gathered.reshape(rows, n, lanes).transpose(1, 0, 2).reshape(n * rows, lanes)

    down_full = stacked(adapter_down_full, adapter_down.shape[2])
    state_in_full = stacked(state_full, state_pad.shape[1])[:, :state_width]

    d_normed_four = lax.psum_scatter(
        matrix_product_transposed(output_gradient, mixer_out_matrix).astype(BF)[None],
        "col",
        scatter_dimension=2,
        tiled=True,
    )[0].astype(F32)

    scale_one = lax.rsqrt(sum_one.reshape(-1) / concat_width + EPS)[:, None]
    norm_one = concat * scale_one
    normed_one = (x_one.astype(F32) * scale_one).astype(BF)
    head_size = 128
    qkv_own = jnp.einsum("tk,iko->ito", normed_one, qkv_t, preferred_element_type=F32)
    heads_here = qkv_own.shape[2] // head_size
    queries, keys_pre, values_pre = [
        qkv_own[i].reshape(length, heads_here, head_size) for i in range(3)
    ]
    attended, attn_back = jax.vjp(
        functools.partial(attention_core, segment=document_numbers), queries, keys_pre, values_pre
    )
    (heads_half,) = exchange(2, [("gather", attended.reshape(length, -1).astype(BF))], 25)
    (attn_sum,) = exchange(
        3, [("rowsum", matrix_product(heads_half, attn_out_flat).astype(BF))], 5
    )
    attn_stream = concat + attn_sum
    x_two, sum_two = exchange(
        4,
        [
            ("gather2", (attn_stream * mlp_gain).astype(BF)),
            ("colsum", pack_rows(jnp.sum(attn_stream * attn_stream, 1))),
        ],
        25,
    )
    scale_two = lax.rsqrt(sum_two.reshape(-1) / concat_width + EPS)[:, None]
    norm_two = attn_stream * scale_two
    normed_two = (x_two.astype(F32) * scale_two).astype(BF)
    adapter_middle = matrix_product(normed_two, down_full)
    gate_up_local = jnp.einsum("tk,iko->ito", normed_two, gate_up_t, preferred_element_type=F32)
    gate_up_local = gate_up_local + jnp.einsum(
        "gb,sbm->sgm", adapter_middle, adapter_up_broad, precision=FULL_PRECISION
    )
    hidden_own = gelu_product(gate_up_local[0], gate_up_local[1]).astype(BF)
    (hidden_half,) = exchange(5, [("gather", hidden_own)], 45)
    (mlp_sum,) = exchange(6, [("rowsum", matrix_product(hidden_half, down_flat).astype(BF))], 5)
    mixed_b = (attn_stream + mlp_sum).astype(BF)
    half_tokens = lax.dynamic_slice_in_dim(mixed_b, row * (length // 2), length // 2, 0)
    (proj_sum,) = exchange(7, [("scatter2", matrix_product(half_tokens, proj_flat).astype(BF))], 15)
    resid = hidden_state_input.astype(F32) + proj_sum
    x_three, sum_three = exchange(
        8,
        [
            ("gather2", (resid * mixer_norm_gain).astype(BF)),
            ("colsum", pack_rows(jnp.sum(resid * resid, 1))),
        ],
        15,
    )
    scale_three = lax.rsqrt(sum_three.reshape(-1) / model_width + EPS)[:, None]
    norm_three = resid * scale_three
    normed_three = (x_three.astype(F32) * scale_three).astype(BF)
    zx_own = jnp.einsum("tk,iko->ito", normed_three, gate_in_t, preferred_element_type=F32)
    bcdt = matrix_product(normed_three, state_in_full)
    state_cols = state_conv_kernel.shape[1]
    heads_own = step_offset_bias.shape[0]
    owner = row * n + col
    step_own = lax.dynamic_slice_in_dim(bcdt, state_cols + owner * heads_own, heads_own, 1)
    docs = jnp.cumsum(document_start_flags) - 1
    bc_conv, bc_back = jax.vjp(
        functools.partial(bc_activate, docs=docs), bcdt[:, :state_cols], state_conv_kernel
    )
    gated, core_back = jax.vjp(
        functools.partial(mixer_core, docs=docs),
        zx_own[1],
        zx_own[0],
        step_own,
        bc_conv,
        mixer_input_kernel,
        step_offset_bias,
        log_decay_rates,
        head_skip_term,
    )
    grad_hat = d_normed_four * gated_norm_gain
    (sums_four,) = exchange(
        9,
        [("allsum", pack_rows(jnp.sum(gated * gated, 1), jnp.sum(grad_hat * gated, 1)))],
        6,
    )
    square_four, cross_four = unpack_rows(sums_four, 2)
    scale_four = lax.rsqrt(square_four / inner_width + EPS)[:, None]
    norm_four = gated * scale_four
    inner_four = cross_four[:, None] * scale_four / inner_width
    d_gated = scale_four * (grad_hat - norm_four * inner_four)
    grad_gated_gain = jnp.sum(d_normed_four * norm_four, 0)
    normed_half = lax.all_gather(
        (norm_four * gated_norm_gain).astype(BF)[None], "col", axis=2, tiled=True
    )[0]
    out_sum = lax.psum(matrix_product(normed_half, mixer_out_matrix).astype(BF), "row")
    block_out = (resid + out_sum.astype(F32)).astype(BF)
    grad_mixer_out_matrix = matmul_tn(normed_half, output_gradient)

    (
        d_x_pre,
        d_gate_z,
        d_step_own,
        d_bc_part,
        grad_mixer_input_kernel,
        grad_step_offset_bias,
        grad_log_decay,
        grad_head_skip,
    ) = core_back(d_gated)
    step_slot = lax.dynamic_update_slice_in_dim(
        jnp.zeros((length, state_width - state_cols), F32), d_step_own, owner * heads_own, 1
    )
    d_bc_pre, grad_state_conv_kernel = bc_back(d_bc_part)
    d_bcdt_b = jnp.concatenate([d_bc_pre, step_slot], 1).astype(BF)
    d_zx_own = jnp.stack([d_gate_z, d_x_pre]).astype(BF)
    partial_three = jnp.einsum(
        "ito,iko->tk", d_zx_own, gate_in_t, preferred_element_type=F32
    ) + matrix_product_transposed(d_bcdt_b, state_in_full)
    cross_three = jnp.sum(d_zx_own.astype(F32) * zx_own, (0, 2)) + jnp.sum(
        d_bcdt_b.astype(F32) * bcdt, 1
    )
    d_normed_three, inner_three = exchange(
        10, [("reduce", partial_three.astype(BF)), ("allsum", pack_rows(cross_three))], 18
    )

    def returned(grad, ident, micros):
        outer, own = grad.shape[0], grad.shape[2]
        shaped = grad.astype(BF).reshape(outer, n, -1, width, own).transpose(1, 0, 2, 3, 4)
        lead = shaped.shape[1] * shaped.shape[2]
        shaped = shaped.reshape(n, lead, width, own)
        share = lax.psum_scatter(shaped, "dp", scatter_dimension=2, tiled=True)
        (back,) = exchange(ident, [("a2a_back", share.reshape(n, -1, own))], micros)
        full = lax.all_gather(
            back.reshape(lead, -1, n * own), "dp", axis=1, tiled=True
        )
        return full.astype(F32)

    def dp_sum(grad):
        return lax.psum(grad.astype(BF), "dp").astype(F32)

    def norm_back(grad_in, inner, normal, scale, gain, count):
        mean = inner.reshape(-1)[:, None] / count
        return scale * (grad_in * gain - normal * mean), jnp.sum(grad_in * normal, 0)

    grad_gate_in = jnp.einsum("tk,ito->iko", normed_three, d_zx_own, preferred_element_type=F32)
    grad_state_in_part = matmul_tn(normed_three, d_bcdt_b)
    d_norm_three, grad_mixer_gain = norm_back(
        d_normed_three, inner_three, norm_three, scale_three, mixer_norm_gain, model_width
    )
    d_resid = output_gradient.astype(F32) + d_norm_three
    (d_resid_full,) = exchange(11, [("gather2", d_resid.astype(BF))], 15)
    grad_projection_matrix = matmul_tn(mixed_b, d_resid_full)
    d_mixed = matrix_product_transposed(d_resid_full, proj_flat)
    d_mixed_b = d_mixed.astype(BF)
    grad_down_matrix = matmul_tn(hidden_half, d_mixed_b)
    (d_hidden_own,) = exchange(
        12, [("scatter", matrix_product_transposed(d_mixed_b, down_flat).astype(BF))], 45
    )
    act_back = jax.vjp(gelu_product, gate_up_local[0], gate_up_local[1])[1]
    grad_gate_up_local = jnp.stack(act_back(d_hidden_own))
    grad_adapter_up = jnp.einsum(
        "mc,ymv->ycv", adapter_middle, grad_gate_up_local, precision=FULL_PRECISION
    )
    middle_part = jnp.einsum(
        "oaj,opj->ap", grad_gate_up_local, adapter_up_broad, precision=FULL_PRECISION
    ).astype(BF)
    d_gate_up_b = grad_gate_up_local.astype(BF)
    partial_two = jnp.einsum(
        "ito,iko->tk", d_gate_up_b, gate_up_t, preferred_element_type=F32
    ) + matrix_product_transposed(middle_part, down_full)
    cross_two = jnp.sum(d_gate_up_b.astype(F32) * gate_up_local, (0, 2))
    d_normed_two, inner_two = exchange(
        13, [("reduce", partial_two.astype(BF)), ("allsum", pack_rows(cross_two))], 28
    )
    grad_gate_up = jnp.einsum("tk,ito->iko", normed_two, d_gate_up_b, preferred_element_type=F32)
    grad_adapter_down_part = matmul_tn(normed_two, middle_part)
    d_norm_two, grad_perceptron_gain = norm_back(
        d_normed_two, inner_two, norm_two, scale_two, mlp_gain, concat_width
    )
    d_attn = d_mixed + d_norm_two
    d_attn_b = d_attn.astype(BF)
    grad_attention_out = matmul_tn(heads_half, d_attn_b)
    (d_heads_own,) = exchange(
        14, [("scatter", matrix_product_transposed(d_attn_b, attn_out_flat).astype(BF))], 25
    )
    d_qkv_b = jnp.stack(
        [g.reshape(length, -1) for g in attn_back(d_heads_own.reshape(length, heads_here, head_size))]
    ).astype(BF)
    partial_one = jnp.einsum("ito,iko->tk", d_qkv_b, qkv_t, preferred_element_type=F32)
    cross_one = jnp.sum(d_qkv_b.astype(F32) * qkv_own, (0, 2))
    grad_qkv = jnp.einsum("tk,ito->iko", normed_one, d_qkv_b, preferred_element_type=F32)
    d_normed_one, inner_one = exchange(
        15, [("reduce", partial_one.astype(BF)), ("allsum", pack_rows(cross_one))], 28
    )
    d_norm_one, grad_attention_gain = norm_back(
        d_normed_one, inner_one, norm_one, scale_one, attn_gain, concat_width
    )
    d_concat = (d_attn + d_norm_one).reshape(length, 2, width)
    grad_hidden = d_resid + d_concat[:, 0]
    grad_embed = d_concat[:, 1]

    grad_gate_in_matrix = returned(grad_gate_in, 16, 15).reshape(gate_in_matrix.shape)
    grad_gate_up_matrix = returned(grad_gate_up, 17, 25).reshape(gate_up_matrix.shape)
    grad_query_key_value = returned(grad_qkv, 18, 20).reshape(query_key_value_matrix.shape)

    def own_features(summed):
        rows = summed.shape[0] // n
        return lax.dynamic_slice_in_dim(summed, col * rows, rows, 0)

    shared = lax.psum(
        (grad_state_in_part.astype(BF), grad_adapter_down_part.astype(BF)), ("dp", "row", "col")
    )
    grad_state_in_matrix = own_features(shared[0]).astype(F32)
    grad_adapter_down = own_features(shared[1]).astype(F32).reshape(adapter_down.shape)
    grad_state_conv_kernel = lax.psum(grad_state_conv_kernel, ("dp", "row", "col"))
    (
        grad_attention_gain,
        grad_perceptron_gain,
        grad_mixer_gain,
        grad_mixer_input_kernel,
        grad_step_offset_bias,
        grad_log_decay,
        grad_head_skip,
        grad_gated_gain,
    ) = lax.psum(
        (
            grad_attention_gain.reshape(attention_norm_gain.shape),
            grad_perceptron_gain.reshape(perceptron_norm_gain.shape),
            grad_mixer_gain,
            grad_mixer_input_kernel,
            grad_step_offset_bias,
            grad_log_decay,
            grad_head_skip,
            grad_gated_gain,
        ),
        "dp",
    )
    return (
        block_out,
        grad_hidden,
        grad_embed,
        grad_attention_gain,
        grad_query_key_value,
        dp_sum(grad_attention_out).reshape(attention_out_matrix.shape),
        grad_perceptron_gain,
        grad_gate_up_matrix,
        grad_adapter_down,
        dp_sum(grad_adapter_up),
        dp_sum(grad_down_matrix).reshape(down_matrix.shape),
        dp_sum(grad_projection_matrix).reshape(projection_matrix.shape),
        grad_mixer_gain,
        grad_gate_in_matrix,
        grad_state_in_matrix,
        grad_mixer_input_kernel,
        grad_state_conv_kernel,
        grad_step_offset_bias,
        grad_log_decay,
        grad_head_skip,
        grad_gated_gain,
        dp_sum(grad_mixer_out_matrix),
    )


def solution(mesh):
    tokens = P("dp", "col")
    spread = ("row", "col")
    return jax.shard_map(
        body,
        mesh=mesh,
        in_specs=(
            tokens,
            tokens,
            P("dp"),
            P("dp"),
            P(None, "col"),
            P(None, None, "col", "row"),
            P("row", None, "col"),
            P(None, "col"),
            P(None, None, "col", "row"),
            P(None, "col", None),
            P(None, None, spread),
            P("row", None, "col"),
            P(None, "col", None),
            P("col"),
            P(None, "col", "row"),
            P("col", None),
            P(None, spread),
            P(),
            P(spread),
            P(spread),
            P(spread),
            P(spread),
            P("row", "col"),
            tokens,
        ),
        out_specs=(
            tokens,
            tokens,
            tokens,
            P(None, "col"),
            P(None, None, "col", "row"),
            P("row", None, "col"),
            P(None, "col"),
            P(None, None, "col", "row"),
            P(None, "col", None),
            P(None, None, spread),
            P("row", None, "col"),
            P(None, "col", None),
            P("col"),
            P(None, "col", "row"),
            P("col", None),
            P(None, spread),
            P(),
            P(spread),
            P(spread),
            P(spread),
            P(spread),
            P("row", "col"),
        ),
        check_vma=False,
    )
```

```python
import functools
import math

import jax
import jax.numpy as jnp
from jax import lax
from jax.experimental import pallas as pl
from jax.experimental.pallas import tpu as pltpu
from jax.sharding import PartitionSpec as P

EPS = 1e-05
FULL_PRECISION = lax.Precision.HIGHEST
BF = jnp.bfloat16
F32 = jnp.float32
MESH = pl.DeviceIdType.MESH


def matrix_product(left, right):
    return jnp.dot(left, right, preferred_element_type=F32)


def matmul_tn(left, right):
    return lax.dot_general(left, right, (((0,), (0,)), ((), ())), preferred_element_type=F32)


def matrix_product_transposed(left, right):
    return lax.dot_general(left, right, (((1,), (1,)), ((), ())), preferred_element_type=F32)


def rope_tables(length, width):
    half = width // 2
    positions = jnp.arange(length).astype(F32)
    rates = jnp.exp(-math.log(10000.0) * jnp.arange(half).astype(F32) / half)
    angles = positions[:, None] * rates[None, :]
    return (jnp.cos(angles)[:, None, :], jnp.sin(angles)[:, None, :])


def rotate(vectors, cosine, sine):
    half = vectors.shape[-1] // 2
    first = vectors[..., :half]
    second = vectors[..., half:]
    return jnp.concatenate([first * cosine - second * sine, first * sine + second * cosine], -1)


def attention_core(queries, keys, values, segment):
    length = queries.shape[0]
    width = queries.shape[2]
    cosine, sine = rope_tables(length, width)
    queries = rotate(queries, cosine, sine)
    keys = rotate(keys, cosine, sine)
    scores = jnp.einsum("qhd,khd->hqk", queries, keys, precision=FULL_PRECISION) / math.sqrt(width)
    places = jnp.arange(length)
    allowed = (places[:, None] >= places[None, :]) & (segment[:, None] == segment[None, :])
    weight_list = jnp.where(allowed[None], jnp.exp(scores), 0.0)
    weight_list = weight_list / jnp.sum(weight_list, -1, keepdims=True)
    return jnp.einsum("hqk,khd->qhd", weight_list, values, precision=FULL_PRECISION)


def conv_causal(signal, kernel, docs):
    total = signal * kernel[0]
    for offset in range(1, kernel.shape[0]):
        shifted = jnp.concatenate(
            [jnp.zeros((offset, signal.shape[1]), signal.dtype), signal[:-offset]], 0
        )
        shifted_docs = jnp.concatenate([jnp.full((offset,), -1, jnp.int32), docs[:-offset]], 0)
        same = (shifted_docs == docs).astype(signal.dtype)[:, None]
        total = total + shifted * kernel[offset] * same
    return total


def bc_activate(bc_pre, kernel, docs):
    return jax.nn.silu(conv_causal(bc_pre, kernel, docs))


def mixer_core(
    x_pre,
    gate_z,
    step_raw,
    bc_conv,
    conv_kernel,
    step_offset_bias,
    log_decay_rates,
    head_skip_term,
    docs,
):
    length = x_pre.shape[0]
    heads = step_raw.shape[1]
    head_dim = x_pre.shape[1] // heads
    state = bc_conv.shape[1] // 2
    inner = jax.nn.silu(conv_causal(x_pre, conv_kernel, docs)).reshape(length, heads, head_dim)
    b_states = bc_conv[:, :state]
    c_states = bc_conv[:, state:]
    step = jax.nn.softplus(step_raw + step_offset_bias)
    rate = -jnp.exp(log_decay_rates) * step
    cumulative = jnp.cumsum(rate, 0)
    places = jnp.arange(length)
    allowed = ((places[:, None] >= places[None, :]) & (docs[:, None] == docs[None, :]))[None]
    gaps = cumulative.T[:, :, None] - cumulative.T[:, None, :]
    decay = jnp.where(allowed, jnp.exp(jnp.where(allowed, gaps, 0.0)), 0.0)
    intersection = jnp.dot(c_states, b_states.T, precision=FULL_PRECISION)
    mixing = decay * intersection[None]
    weighted = inner * step[:, :, None]
    outputs = jnp.einsum("hts,shp->thp", mixing, weighted, precision=FULL_PRECISION)
    outputs = outputs + head_skip_term[None, :, None] * inner
    return outputs.reshape(length, heads * head_dim) * jax.nn.silu(gate_z)


def gelu_product(gate_preact, up_preact):
    return jax.nn.gelu(gate_preact, approximate=True) * up_preact


def _window(index, size):
    return pl.ds(pl.multiple_of(index * size, size), size)


def _add_rows(rows, write):
    chunk = 64 if rows % 64 == 0 else rows
    if rows == chunk:
        write(pl.ds(0, rows))
        return

    def step(i, carry):
        write(pl.ds(pl.multiple_of(i * chunk, chunk), chunk))
        return carry

    lax.fori_loop(0, rows // chunk, step, 0)


def _remote(src, dst, send, recv, device):
    copy = pltpu.make_async_remote_copy(
        src_ref=src,
        dst_ref=dst,
        send_sem=send,
        recv_sem=recv,
        device_id=device,
        device_id_type=MESH,
    )
    copy.start()
    return copy


class Env:
    def __init__(self, n, replicas):
        self.n = n
        self.replicas = replicas
        self.dp = lax.axis_index("dp")
        self.col = lax.axis_index("col")
        self.row = lax.axis_index("row")
        self.sibling = {"row": 1 - self.row}

    def peer(self, k):
        return {"col": lax.rem(self.col + k, self.n)}

    def replica(self, k):
        return {"dp": lax.rem(self.dp + k, self.replicas)}


class Relay:

    def __init__(self, env, where, send, recv, direction):
        self.env, self.where, self.direction = env, where, direction
        self.send, self.recv = send, recv
        self.base = 0 if direction > 0 else env.n - 1
        self.neighbour = {"col": jnp.clip(env.col + direction, 0, env.n - 1)}

    def copy(self, step, source):
        i = self.base + step
        return pltpu.make_async_remote_copy(
            src_ref=source,
            dst_ref=self.where(self.owner(step)),
            send_sem=self.send.at[i],
            recv_sem=self.recv.at[i],
            device_id=self.neighbour,
            device_id_type=MESH,
        )

    def owner(self, step):
        owner = self.env.col - self.direction * step
        return jnp.clip(owner, 0, self.env.n - 1)

    def place(self):
        return self.env.col if self.direction > 0 else self.env.n - 1 - self.env.col

    def sends(self, step):
        return (self.place() < self.env.n - 1) & (self.place() >= step)

    def receives(self, step):
        return self.place() > step

    def start(self, step, source):
        @pl.when(self.sends(step))
        def _():
            self.copy(step, source).start()

    def arrived(self, step, then=None):
        @pl.when(self.receives(step))
        def _():
            part = self.where(self.owner(step + 1))
            pltpu.make_async_remote_copy(
                src_ref=part,
                dst_ref=part,
                send_sem=self.send.at[self.base + step],
                recv_sem=self.recv.at[self.base + step],
                device_id=self.neighbour,
                device_id_type=MESH,
            ).wait_recv()
            if then is not None:
                then(part, self.base + step)

    def sent(self, step, source):
        @pl.when(self.sends(step))
        def _():
            self.copy(step, source).wait_send()


def run_gather(env, x, o, send, recv, local):
    width = x.shape[1]

    def where(owner):
        return o.at[:, _window(owner, width)]

    own = pltpu.make_async_copy(x, where(env.col), local.at[0])
    ways = [Relay(env, where, send, recv, d) for d in (1, -1)]
    for way in ways:
        way.start(0, x)
    own.start()
    yield
    for step in range(env.n - 1):
        for way in ways:
            way.arrived(step)
            if step < env.n - 2:
                way.start(step + 1, where(way.owner(step + 1)))
        yield
    own.wait()
    for step in range(env.n - 1):
        for way in ways:
            way.sent(step, x)


def run_gather2(env, x, o, send, recv, local, send2, recv2):
    width = x.shape[1]
    half = x.shape[0] // 2
    mine = _window(env.row, half)

    def where(owner):
        return o.at[mine, _window(owner, width)]

    source = x.at[mine, :]

    def across(part, i):
        return pltpu.make_async_remote_copy(
            src_ref=part,
            dst_ref=part,
            send_sem=send2.at[i],
            recv_sem=recv2.at[i],
            device_id=env.sibling,
            device_id_type=MESH,
        )

    def pass_on(part, i):
        across(part, i).start()

    own = pltpu.make_async_copy(x, o.at[:, _window(env.col, width)], local.at[0])
    ways = [Relay(env, where, send, recv, d) for d in (1, -1)]
    for way in ways:
        way.start(0, source)
    own.start()
    yield
    for step in range(env.n - 1):
        for way in ways:
            way.arrived(step, pass_on)
            if step < env.n - 2:
                way.start(step + 1, where(way.owner(step + 1)))
        yield
    own.wait()
    for step in range(env.n - 1):
        for way in ways:
            way.sent(step, source)

            @pl.when(way.receives(step))
            def _(way=way, step=step):
                part = where(way.owner(step + 1))
                across(part, way.base + step).wait()


def run_scatter(env, p, o, buffer, send, recv):
    rows, width = o.shape
    copies = [
        _remote(
            p.at[:, _window(lax.rem(env.col + k, env.n), width)],
            buffer.at[k - 1],
            send.at[k - 1],
            recv.at[k - 1],
            env.peer(k),
        )
        for k in range(1, env.n)
    ]
    yield
    for copy in copies:
        copy.wait()

    def write(part):
        total = p[part, _window(env.col, width)].astype(F32)
        for k in range(env.n - 1):
            total = total + buffer[k, part, :].astype(F32)
        o[part, :] = total

    _add_rows(rows, write)


def run_scatter2(env, p, o, buffer, send, recv, send2, recv2):
    rows, width = p.shape[0], o.shape[1]
    size = rows // 2
    copies = []
    for c in range(2):
        for k in range(1, env.n):
            i = c * (env.n - 1) + k - 1
            part = pl.ds(c * size, size)
            copies.append(
                _remote(
                    p.at[part, _window(lax.rem(env.col + k, env.n), width)],
                    buffer.at[k - 1, part, :],
                    send.at[i],
                    recv.at[i],
                    env.peer(k),
                )
            )
    yield
    first = env.row * rows
    onward = []
    for c in range(2):
        for k in range(1, env.n):
            copies[c * (env.n - 1) + k - 1].wait()

        def write(part, c=c):
            source = pl.ds(pl.multiple_of(c * size + part.start, 16), part.size)
            total = p[source, _window(env.col, width)].astype(F32)
            for k in range(env.n - 1):
                total = total + buffer[k, source, :].astype(F32)
            target = pl.ds(pl.multiple_of(first + c * size + part.start, 8), part.size)
            o[target, :] = total

        _add_rows(size, write)
        half = o.at[_window(env.row * 2 + c, size), :]
        onward.append(_remote(half, half, send2.at[c], recv2.at[c], env.sibling))
    yield
    for copy in onward:
        copy.wait()


def run_reduce(env, p, o, pairs, sums, buffer, send, recv, send2, recv2, send3, recv3):
    rows, width = o.shape
    half = rows // 2
    size = half // 2
    other = _window(1 - env.row, half)
    order = [(k + 1) % env.n for k in range(env.n)]
    first = []
    for i, k in enumerate(order):
        piece = _window(lax.rem(env.col + k, env.n), width)
        first.append(
            _remote(p.at[other, piece], pairs.at[i], send.at[i], recv.at[i], env.sibling)
        )
    yield
    start = env.row * half
    copies = {}
    for i, k in enumerate(order):
        first[i].wait()
        piece = _window(lax.rem(env.col + k, env.n), width)

        def write(part, i=i, piece=piece):
            source = pl.ds(pl.multiple_of(start + part.start, 16), part.size)
            total = p[source, piece].astype(F32) + pairs[i, part, :].astype(F32)
            sums[i, part, :] = total.astype(sums.dtype)

        _add_rows(half, write)
        if k:
            for c in range(2):
                part = pl.ds(c * size, size)
                j = 2 * i + c
                copies[j] = _remote(
                    sums.at[i, part, :],
                    buffer.at[i, part, :],
                    send2.at[j],
                    recv2.at[j],
                    env.peer(k),
                )
    yield
    onward = []
    for c in range(2):
        for i in range(env.n - 1):
            copies[2 * i + c].wait()

        def finish(part, c=c):
            source = pl.ds(pl.multiple_of(c * size + part.start, 16), part.size)
            total = sums[env.n - 1, source, :].astype(F32)
            for k in range(env.n - 1):
                total = total + buffer[k, source, :].astype(F32)
            target = pl.ds(pl.multiple_of(start + c * size + part.start, 8), part.size)
            o[target, :] = total

        _add_rows(size, finish)
        part = o.at[_window(env.row * 2 + c, size), :]
        onward.append(_remote(part, part, send3.at[c], recv3.at[c], env.sibling))
    yield
    for copy in onward:
        copy.wait()


def run_a2a(env, x, o, send, recv, local):
    for _ in range(env.n - 2):
        yield
    width = o.shape[3]
    copies = [
        _remote(
            x.at[:, :, _window(lax.rem(env.col + k, env.n), width)],
            o.at[:, env.col],
            send.at[k - 1],
            recv.at[k - 1],
            env.peer(k),
        )
        for k in range(1, env.n)
    ]
    own = pltpu.make_async_copy(
        x.at[:, :, _window(env.col, width)], o.at[:, env.col], local.at[0]
    )
    own.start()
    yield
    own.wait()
    for copy in copies:
        copy.wait()


def run_a2a_back(delay, env, x, o, send, recv, local):
    for _ in range(delay):
        yield
    here = o.at[:, :, _window(env.col, x.shape[3])]
    copies = [
        _remote(
            x.at[:, lax.rem(env.col + k, env.n)],
            here,
            send.at[k - 1],
            recv.at[k - 1],
            env.peer(k),
        )
        for k in range(1, env.n)
    ]
    own = pltpu.make_async_copy(x.at[:, env.col], here, local.at[0])
    own.start()
    yield
    own.wait()
    for copy in copies:
        copy.wait()


def run_dpscatter(env, x, o, buffer, send, recv):
    groups, rows, _ = o.shape
    copies = [
        _remote(
            x.at[:, _window(lax.rem(env.dp + k, env.replicas), rows), :],
            buffer.at[k - 1],
            send.at[k - 1],
            recv.at[k - 1],
            env.replica(k),
        )
        for k in range(1, env.replicas)
    ]
    yield
    for copy in copies:
        copy.wait()
    start = env.dp * rows
    chunk = 64 if rows % 64 == 0 else rows
    steps = rows // chunk

    def step(i, carry):
        group = i // steps
        first = (i % steps) * chunk
        source = pl.ds(pl.multiple_of(start + first, 16), chunk)
        part = pl.ds(pl.multiple_of(first, 16), chunk)
        total = x[group, source, :].astype(F32)
        for k in range(env.replicas - 1):
            total = total + buffer[k, group, part, :].astype(F32)
        o[group, part, :] = total.astype(o.dtype)
        return carry

    lax.fori_loop(0, groups * steps, step, 0)


def run_dpgather(env, x, o, send, recv, local):
    here = o.at[:, _window(env.dp, x.shape[1]), :]
    copies = [
        _remote(x, here, send.at[k - 1], recv.at[k - 1], env.replica(k))
        for k in range(1, env.replicas)
    ]
    own = pltpu.make_async_copy(x, here, local.at[0])
    own.start()
    yield
    own.wait()
    for copy in copies:
        copy.wait()


def run_dpsum(env, s, o, buffer, send, recv, local):
    copies = [
        _remote(s, buffer.at[env.dp], send.at[k - 1], recv.at[k - 1], env.replica(k))
        for k in range(1, env.replicas)
    ]
    own = pltpu.make_async_copy(s, buffer.at[env.dp], local.at[0])
    own.start()
    yield
    own.wait()
    for copy in copies:
        copy.wait()
    total = buffer[0]
    for i in range(1, env.replicas):
        total = total + buffer[i]
    o[...] = total


def run_rowsum(env, p, o, buffer, send, recv):
    copy = _remote(p, buffer, send.at[0], recv.at[0], env.sibling)
    yield
    copy.wait()

    def write(part):
        o[part, :] = p[part, :].astype(F32) + buffer[part, :].astype(F32)

    _add_rows(p.shape[0], write)


def run_sum(env, s, o, buffer, send, recv, local):
    both = buffer.shape[0] > env.n
    mine = env.row * env.n + env.col if both else env.col
    copies = []
    for r in range(2 if both else 1):
        for k in range(env.n):
            if r == 0 and k == 0:
                continue
            device = dict(env.peer(k)) if k else {}
            if r:
                device["row"] = 1 - env.row
            index = r * env.n + k - 1
            copies.append(_remote(s, buffer.at[mine], send.at[index], recv.at[index], device))
    own = pltpu.make_async_copy(s, buffer.at[mine], local.at[0])
    own.start()
    yield
    own.wait()
    for copy in copies:
        copy.wait()
    total = buffer[0]
    for i in range(1, buffer.shape[0]):
        total = total + buffer[i]
    o[...] = total


def plan(kind, x, n, replicas):
    dma = pltpu.SemaphoreType.DMA
    shape = x.shape
    three = dma((n - 1,))
    one, two = dma((1,)), dma((2,))
    twice = dma((2 * (n - 1),))
    if kind == "gather":
        return run_gather, (shape[0], n * shape[1]), x.dtype, [twice, twice, one]
    if kind == "gather2":
        scratch = [twice, twice, one, twice, twice]
        return run_gather2, (shape[0], n * shape[1]), x.dtype, scratch
    if kind == "scatter":
        out = (shape[0], shape[1] // n)
        return run_scatter, out, F32, [pltpu.VMEM((n - 1,) + out, x.dtype), three, three]
    if kind == "scatter2":
        part = (shape[0], shape[1] // n)
        out = (2 * shape[0], shape[1] // n)
        scratch = [pltpu.VMEM((n - 1,) + part, x.dtype), twice, twice, two, two]
        return run_scatter2, out, F32, scratch
    if kind == "reduce":
        out = (shape[0], shape[1] // n)
        part = (shape[0] // 2, shape[1] // n)
        four = dma((n,))
        scratch = [
            pltpu.VMEM((n,) + part, x.dtype),
            pltpu.VMEM((n,) + part, x.dtype),
            pltpu.VMEM((n - 1,) + part, x.dtype),
            four,
            four,
            twice,
            twice,
            two,
            two,
        ]
        return run_reduce, out, F32, scratch
    if kind == "a2a":
        return run_a2a, (shape[0], n, shape[1], shape[2] // n), x.dtype, [three, three, one]
    if kind.startswith("a2a_back"):
        delay = {"a2a_back": 0, "a2a_back1": 1, "a2a_back2": n - 2}[kind]
        run = functools.partial(run_a2a_back, delay)
        return run, (shape[0], shape[2], n * shape[3]), x.dtype, [three, three, one]
    if kind.startswith("dp"):
        others = dma((replicas - 1,))
        if kind == "dpscatter":
            out = (shape[0], shape[1] // replicas, shape[2])
            return run_dpscatter, out, x.dtype, [
                pltpu.VMEM((replicas - 1,) + out, x.dtype),
                others,
                others,
            ]
        if kind == "dpgather":
            out = (shape[0], shape[1] * replicas, shape[2])
            return run_dpgather, out, x.dtype, [others, others, one]
        scratch = [pltpu.VMEM((replicas,) + shape, x.dtype), others, others, one]
        return run_dpsum, shape, F32, scratch
    if kind == "rowsum":
        return run_rowsum, shape, F32, [pltpu.VMEM(shape, x.dtype), one, one]
    members = n if kind == "colsum" else 2 * n
    many = dma((members - 1,))
    return run_sum, shape, F32, [pltpu.VMEM((members,) + shape, x.dtype), many, many, one]


def exchange(ident, items, micros):
    n = lax.axis_size("col")
    replicas = lax.axis_size("dp")
    plans = [plan(kind, x, n, replicas) for kind, x in items]
    kinds = {kind for kind, _ in items}
    count = len(items)
    use_all = "allsum" in kinds
    use_dp = any(kind.startswith("dp") for kind in kinds)
    use_col = use_all or any(kind != "rowsum" and not kind.startswith("dp") for kind in kinds)
    use_row = use_all or bool(kinds & {"rowsum", "gather2", "scatter2", "reduce"})

    def kernel(*refs):
        env = Env(n, replicas)
        barrier = pltpu.get_barrier_semaphore()
        targets = []
        if use_col:
            targets += [env.peer(k) for k in range(1, n)]
        if use_row:
            targets.append(env.sibling)
        if use_all:
            targets += [{**env.peer(k), **env.sibling} for k in range(1, n)]
        if use_dp:
            targets += [env.replica(k) for k in range(1, replicas)]
        for target in targets:
            pl.semaphore_signal(barrier, inc=1, device_id=target, device_id_type=MESH)
        pl.semaphore_wait(barrier, len(targets))
        position = 2 * count
        running = []
        for i in range(count):
            size = len(plans[i][3])
            scratch = refs[position : position + size]
            position += size
            running.append(plans[i][0](env, refs[i], refs[count + i], *scratch))
        while running:
            alive = []
            for item in running:
                try:
                    next(item)
                except StopIteration:
                    continue
                alive.append(item)
            running = alive

    vmem = pl.BlockSpec(memory_space=pltpu.VMEM)
    return pl.pallas_call(
        kernel,
        out_shape=[jax.ShapeDtypeStruct(p[1], p[2]) for p in plans],
        in_specs=[vmem] * count,
        out_specs=[vmem] * count,
        scratch_shapes=[s for p in plans for s in p[3]],
        compiler_params=pltpu.CompilerParams(collective_id=ident, has_side_effects=True),
        cost_estimate=pl.CostEstimate(
            flops=0, bytes_accessed=int(micros * 3000000), transcendentals=0
        ),
        name="exchange_%d" % ident,
    )(*[x for _, x in items])


def pack_rows(*vectors):
    return jnp.concatenate([v.reshape(-1, 128) for v in vectors], 0)


def unpack_rows(packed, count):
    return [part.reshape(-1) for part in jnp.split(packed, count, 0)]


def body(
    hidden_state_input,
    initial_token_embedding,
    document_numbers,
    document_start_flags,
    attention_norm_gain,
    query_key_value_matrix,
    attention_out_matrix,
    perceptron_norm_gain,
    gate_up_matrix,
    adapter_down,
    adapter_up,
    down_matrix,
    projection_matrix,
    mixer_norm_gain,
    gate_in_matrix,
    state_in_matrix,
    mixer_input_kernel,
    state_conv_kernel,
    step_offset_bias,
    log_decay_rates,
    head_skip_term,
    gated_norm_gain,
    mixer_out_matrix,
    output_gradient,
):
    n = lax.axis_size("col")
    replicas = lax.axis_size("dp")
    dp, row, col = lax.axis_index("dp"), lax.axis_index("row"), lax.axis_index("col")
    length, width = hidden_state_input.shape
    local_width = 2 * width
    model_width = n * width
    concat_width = n * local_width
    inner_width = gated_norm_gain.shape[0] * 2 * n

    def my_rows(weight):
        share = weight.shape[2] // replicas
        part = lax.dynamic_slice_in_dim(weight, dp * share, share, 2)
        return part.reshape(weight.shape[0], -1, weight.shape[3])

    def spread(pieces, inner):
        outer, own = pieces.shape[0], pieces.shape[3]
        shaped = pieces.reshape(outer, n, inner, -1, own)
        full = lax.all_gather(shaped, "dp", axis=3, tiled=True)
        return full.reshape(outer, -1, own)

    def after(value, *others):
        return lax.optimization_barrier((value,) + others)[0]

    attn_gain = attention_norm_gain.reshape(local_width)
    mlp_gain = perceptron_norm_gain.reshape(local_width)
    attn_out_flat = attention_out_matrix.reshape(attention_out_matrix.shape[0], local_width)
    down_flat = down_matrix.reshape(down_matrix.shape[0], local_width)
    proj_flat = projection_matrix.reshape(local_width, projection_matrix.shape[2])
    adapter_up_broad = adapter_up.astype(F32)
    state_width = state_in_matrix.shape[1]
    state_pad = jnp.pad(state_in_matrix, ((0, 0), (0, -state_width % 128)))

    (qkv_pieces,) = exchange(0, [("a2a", my_rows(query_key_value_matrix))], 20)
    qkv_t = spread(qkv_pieces, 2)

    concat = (
        jnp.stack([hidden_state_input, initial_token_embedding], 1)
        .astype(F32)
        .reshape(length, local_width)
    )
    x_one, sum_one, gate_up_pieces, gate_in_pieces, adapter_down_full, state_full = exchange(
        1,
        [
            ("gather2", after((concat * attn_gain).astype(BF), qkv_pieces)),
            ("colsum", pack_rows(jnp.sum(concat * concat, 1))),
            ("a2a", my_rows(gate_up_matrix)),
            ("a2a", my_rows(gate_in_matrix[:, None])),
            ("gather2", adapter_down.reshape(local_width, -1)),
            ("gather2", state_pad),
        ],
        60,
    )

    gate_up_t = spread(after(gate_up_pieces, qkv_t), 2)
    gate_in_t = spread(after(gate_in_pieces, gate_up_t), 1)

    def stacked(gathered, lanes):
        rows = gathered.shape[0]
        return gathered.reshape(rows, n, lanes).transpose(1, 0, 2).reshape(n * rows, lanes)

    down_full = stacked(adapter_down_full, adapter_down.shape[2])
    state_in_full = stacked(state_full, state_pad.shape[1])[:, :state_width]

    d_normed_four = lax.psum_scatter(
        matrix_product_transposed(output_gradient, mixer_out_matrix).astype(BF)[None],
        "col",
        scatter_dimension=2,
        tiled=True,
    )[0].astype(F32)

    scale_one = lax.rsqrt(sum_one.reshape(-1) / concat_width + EPS)[:, None]
    norm_one = concat * scale_one
    normed_one = (x_one.astype(F32) * scale_one).astype(BF)
    head_size = 128
    qkv_own = jnp.einsum("tk,iko->ito", normed_one, qkv_t, preferred_element_type=F32)
    heads_here = qkv_own.shape[2] // head_size
    queries, keys_pre, values_pre = [
        qkv_own[i].reshape(length, heads_here, head_size) for i in range(3)
    ]
    attended, attn_back = jax.vjp(
        functools.partial(attention_core, segment=document_numbers), queries, keys_pre, values_pre
    )
    (heads_half,) = exchange(2, [("gather", attended.reshape(length, -1).astype(BF))], 25)
    (attn_sum,) = exchange(
        3, [("rowsum", matrix_product(heads_half, attn_out_flat).astype(BF))], 5
    )
    attn_stream = concat + attn_sum
    x_two, sum_two = exchange(
        4,
        [
            ("gather2", (attn_stream * mlp_gain).astype(BF)),
            ("colsum", pack_rows(jnp.sum(attn_stream * attn_stream, 1))),
        ],
        25,
    )
    scale_two = lax.rsqrt(sum_two.reshape(-1) / concat_width + EPS)[:, None]
    norm_two = attn_stream * scale_two
    normed_two = (x_two.astype(F32) * scale_two).astype(BF)
    adapter_middle = matrix_product(normed_two, down_full)
    gate_up_local = jnp.einsum("tk,iko->ito", normed_two, gate_up_t, preferred_element_type=F32)
    gate_up_local = gate_up_local + jnp.einsum(
        "gb,sbm->sgm", adapter_middle, adapter_up_broad, precision=FULL_PRECISION
    )
    hidden_own = gelu_product(gate_up_local[0], gate_up_local[1]).astype(BF)
    (hidden_half,) = exchange(5, [("gather", hidden_own)], 45)
    (mlp_sum,) = exchange(6, [("rowsum", matrix_product(hidden_half, down_flat).astype(BF))], 5)
    mixed_b = (attn_stream + mlp_sum).astype(BF)
    half_tokens = lax.dynamic_slice_in_dim(mixed_b, row * (length // 2), length // 2, 0)
    (proj_sum,) = exchange(7, [("scatter2", matrix_product(half_tokens, proj_flat).astype(BF))], 15)
    resid = hidden_state_input.astype(F32) + proj_sum
    x_three, sum_three = exchange(
        8,
        [
            ("gather2", (resid * mixer_norm_gain).astype(BF)),
            ("colsum", pack_rows(jnp.sum(resid * resid, 1))),
        ],
        15,
    )
    scale_three = lax.rsqrt(sum_three.reshape(-1) / model_width + EPS)[:, None]
    norm_three = resid * scale_three
    normed_three = (x_three.astype(F32) * scale_three).astype(BF)
    zx_own = jnp.einsum("tk,iko->ito", normed_three, gate_in_t, preferred_element_type=F32)
    bcdt = matrix_product(normed_three, state_in_full)
    state_cols = state_conv_kernel.shape[1]
    heads_own = step_offset_bias.shape[0]
    owner = row * n + col
    step_own = lax.dynamic_slice_in_dim(bcdt, state_cols + owner * heads_own, heads_own, 1)
    docs = jnp.cumsum(document_start_flags) - 1
    bc_conv, bc_back = jax.vjp(
        functools.partial(bc_activate, docs=docs), bcdt[:, :state_cols], state_conv_kernel
    )
    gated, core_back = jax.vjp(
        functools.partial(mixer_core, docs=docs),
        zx_own[1],
        zx_own[0],
        step_own,
        bc_conv,
        mixer_input_kernel,
        step_offset_bias,
        log_decay_rates,
        head_skip_term,
    )
    grad_hat = d_normed_four * gated_norm_gain
    (sums_four,) = exchange(
        9,
        [("allsum", pack_rows(jnp.sum(gated * gated, 1), jnp.sum(grad_hat * gated, 1)))],
        6,
    )
    square_four, cross_four = unpack_rows(sums_four, 2)
    scale_four = lax.rsqrt(square_four / inner_width + EPS)[:, None]
    norm_four = gated * scale_four
    inner_four = cross_four[:, None] * scale_four / inner_width
    d_gated = scale_four * (grad_hat - norm_four * inner_four)
    grad_gated_gain = jnp.sum(d_normed_four * norm_four, 0)
    normed_half = lax.all_gather(
        (norm_four * gated_norm_gain).astype(BF)[None], "col", axis=2, tiled=True
    )[0]

    (
        d_x_pre,
        d_gate_z,
        d_step_own,
        d_bc_part,
        grad_mixer_input_kernel,
        grad_step_offset_bias,
        grad_log_decay,
        grad_head_skip,
    ) = core_back(d_gated)
    step_slot = lax.dynamic_update_slice_in_dim(
        jnp.zeros((length, state_width - state_cols), F32), d_step_own, owner * heads_own, 1
    )
    d_bc_pre, grad_state_conv_kernel = bc_back(d_bc_part)
    d_bcdt_b = jnp.concatenate([d_bc_pre, step_slot], 1).astype(BF)
    d_zx_own = jnp.stack([d_gate_z, d_x_pre]).astype(BF)
    partial_three = jnp.einsum(
        "ito,iko->tk", d_zx_own, gate_in_t, preferred_element_type=F32
    ) + matrix_product_transposed(d_bcdt_b, state_in_full)
    cross_three = jnp.sum(d_zx_own.astype(F32) * zx_own, (0, 2)) + jnp.sum(
        d_bcdt_b.astype(F32) * bcdt, 1
    )
    grad_gate_in = jnp.einsum("tk,ito->iko", normed_three, d_zx_own, preferred_element_type=F32)

    def split_features(grad, inner):
        outer, own = grad.shape[0], grad.shape[2]
        return grad.astype(BF).reshape(outer, n, inner, -1, own)

    def grouped(grad, inner):
        groups = split_features(grad, inner)
        return groups.reshape((-1,) + groups.shape[3:])

    def ungrouped(share, outer):
        return share.reshape(outer, n, -1, share.shape[2])

    def share_of(grad, inner):
        share = lax.psum_scatter(
            split_features(grad, inner), "dp", scatter_dimension=3, tiled=True
        )
        return share.reshape(share.shape[0], n, -1, share.shape[4])

    def joined(back, inner):
        shaped = back.reshape(back.shape[0], inner, -1, back.shape[2])
        return lax.all_gather(shaped, "dp", axis=2, tiled=True)

    d_normed_three, inner_three, gate_in_share = exchange(
        10,
        [
            ("reduce", partial_three.astype(BF)),
            ("allsum", pack_rows(cross_three)),
            ("dpscatter", grouped(grad_gate_in, 1)),
        ],
        25,
    )

    def norm_back(grad_in, inner, normal, scale, gain, count):
        mean = inner.reshape(-1)[:, None] / count
        return scale * (grad_in * gain - normal * mean), jnp.sum(grad_in * normal, 0)

    grad_state_in_part = matmul_tn(normed_three, d_bcdt_b)
    d_norm_three, grad_mixer_gain = norm_back(
        d_normed_three, inner_three, norm_three, scale_three, mixer_norm_gain, model_width
    )
    d_resid = output_gradient.astype(F32) + d_norm_three
    d_resid_full, conv_sum, gate_in_back = exchange(
        11,
        [
            ("gather2", d_resid.astype(BF)),
            ("allsum", grad_state_conv_kernel),
            ("a2a_back2", ungrouped(gate_in_share, 2)),
        ],
        28,
    )
    gate_in_wide = joined(gate_in_back, 1)
    grad_proj = matmul_tn(mixed_b, d_resid_full).astype(BF)
    d_mixed = matrix_product_transposed(d_resid_full, proj_flat)
    d_mixed_b = d_mixed.astype(BF)
    grad_down = matmul_tn(hidden_half, d_mixed_b).astype(BF)
    partial_hidden = matrix_product_transposed(d_mixed_b, down_flat).astype(BF)
    (d_hidden_own,) = exchange(
        12, [("scatter", after(partial_hidden, grad_proj, grad_down))], 50
    )
    proj_full, down_full_grad = lax.psum((grad_proj, grad_down), "dp")
    act_back = jax.vjp(gelu_product, gate_up_local[0], gate_up_local[1])[1]
    grad_gate_up_local = jnp.stack(act_back(d_hidden_own))
    grad_adapter_up = jnp.einsum(
        "mc,ymv->ycv", adapter_middle, grad_gate_up_local, precision=FULL_PRECISION
    )
    middle_part = jnp.einsum(
        "oaj,opj->ap", grad_gate_up_local, adapter_up_broad, precision=FULL_PRECISION
    ).astype(BF)
    d_gate_up_b = grad_gate_up_local.astype(BF)
    partial_two = jnp.einsum(
        "ito,iko->tk", d_gate_up_b, gate_up_t, preferred_element_type=F32
    ) + matrix_product_transposed(middle_part, down_full)
    cross_two = jnp.sum(d_gate_up_b.astype(F32) * gate_up_local, (0, 2))
    grad_gate_up = jnp.einsum(
        "tk,ito->iko", normed_two, d_gate_up_b, preferred_element_type=F32
    ).astype(BF)
    gate_up_share = share_of(grad_gate_up, 2)
    d_normed_two, inner_two = exchange(
        13,
        [
            ("reduce", after(partial_two.astype(BF), grad_gate_up)),
            ("allsum", pack_rows(cross_two)),
        ],
        30,
    )
    grad_adapter_down_part = matmul_tn(normed_two, middle_part).astype(BF)

    def by_owner(part):
        lanes = part.shape[1] + -part.shape[1] % 128
        padded = jnp.pad(part, ((0, 0), (0, lanes - part.shape[1])))
        return padded.reshape(n, -1, lanes).transpose(1, 0, 2).reshape(-1, n * lanes)
    d_norm_two, grad_perceptron_gain = norm_back(
        d_normed_two, inner_two, norm_two, scale_two, mlp_gain, concat_width
    )
    d_attn = d_mixed + d_norm_two
    d_attn_b = d_attn.astype(BF)
    grad_attention_out = matmul_tn(heads_half, d_attn_b).astype(BF)
    grad_up_flat = grad_adapter_up.astype(BF).reshape(-1, grad_adapter_up.shape[2])
    grad_mixer_out = matmul_tn(after(normed_half, d_normed_two), output_gradient).astype(BF)
    (
        adapter_down_sum,
        state_in_sum,
        gate_up_back,
        d_heads_own,
    ) = exchange(
        14,
        [
            ("reduce", by_owner(grad_adapter_down_part)),
            ("reduce", by_owner(grad_state_in_part.astype(BF))),
            ("a2a_back1", gate_up_share),
            (
                "scatter",
                after(
                    matrix_product_transposed(d_attn_b, attn_out_flat).astype(BF),
                    proj_full,
                    down_full_grad,
                    grad_mixer_out,
                    grad_attention_out,
                    grad_up_flat,
                    gate_in_wide,
                ),
            ),
        ],
        50,
    )
    gate_up_wide = joined(gate_up_back, 2)
    out_full, attn_out_full, up_full = lax.psum(
        lax.optimization_barrier(
            (grad_mixer_out, grad_attention_out, grad_up_flat, proj_full, down_full_grad)
        )[:3],
        "dp",
    )
    d_qkv_b = jnp.stack(
        [g.reshape(length, -1) for g in attn_back(d_heads_own.reshape(length, heads_here, head_size))]
    ).astype(BF)
    partial_one = jnp.einsum("ito,iko->tk", d_qkv_b, qkv_t, preferred_element_type=F32)
    cross_one = jnp.sum(d_qkv_b.astype(F32) * qkv_own, (0, 2))
    grad_qkv = jnp.einsum("tk,ito->iko", normed_one, d_qkv_b, preferred_element_type=F32)
    (
        d_normed_one,
        inner_one,
        qkv_share,
        adapter_down_share,
        state_in_share,
        out_sum,
    ) = exchange(
        15,
        [
            ("reduce", partial_one.astype(BF)),
            ("allsum", pack_rows(cross_one)),
            ("dpscatter", grouped(grad_qkv, 2)),
            ("dpscatter", adapter_down_sum.astype(BF)[None]),
            ("dpscatter", state_in_sum.astype(BF)[None]),
            ("rowsum", matrix_product(after(normed_half, d_normed_two), mixer_out_matrix).astype(BF)),
        ],
        50,
    )
    d_norm_one, grad_attention_gain = norm_back(
        d_normed_one, inner_one, norm_one, scale_one, attn_gain, concat_width
    )
    d_concat = (d_attn + d_norm_one).reshape(length, 2, width)
    grad_hidden = d_resid + d_concat[:, 0]
    grad_embed = d_concat[:, 1]

    small = (
        grad_attention_gain,
        grad_perceptron_gain,
        grad_mixer_gain,
        grad_mixer_input_kernel,
        grad_step_offset_bias,
        grad_log_decay,
        grad_head_skip,
        grad_gated_gain,
        conv_sum,
    )
    flat = jnp.concatenate([value.reshape(-1) for value in small])
    packed = jnp.pad(flat, (0, -flat.size % 1024)).reshape(-1, 128)
    outer = query_key_value_matrix.shape[0]
    qkv_back, adapter_down_sum, state_in_sum, packed_sum = exchange(
        16,
        [
            (
                "a2a_back",
                after(ungrouped(qkv_share, outer), gate_up_wide, out_full, attn_out_full),
            ),
            ("dpgather", adapter_down_share),
            ("dpgather", state_in_share),
            ("dpsum", packed),
        ],
        20,
    )
    grad_query_key_value = joined(qkv_back, 2)
    block_out = (resid + after(out_sum, qkv_back)).astype(BF)
    summed, position = [], 0
    for value in small:
        part = packed_sum.reshape(-1)[position : position + value.size]
        summed.append(part.reshape(value.shape))
        position += value.size
    (
        grad_attention_gain,
        grad_perceptron_gain,
        grad_mixer_gain,
        grad_mixer_input_kernel,
        grad_step_offset_bias,
        grad_log_decay,
        grad_head_skip,
        grad_gated_gain,
        grad_state_conv_kernel,
    ) = summed

    def widened(value, like):
        return after(value, qkv_back).astype(F32).reshape(like.shape)

    return (
        block_out,
        grad_hidden,
        grad_embed,
        grad_attention_gain.reshape(attention_norm_gain.shape),
        grad_query_key_value.astype(F32).reshape(query_key_value_matrix.shape),
        widened(attn_out_full, attention_out_matrix),
        grad_perceptron_gain.reshape(perceptron_norm_gain.shape),
        widened(gate_up_wide, gate_up_matrix),
        widened(adapter_down_sum, adapter_down),
        widened(up_full, adapter_up),
        widened(down_full_grad, down_matrix),
        widened(proj_full, projection_matrix),
        grad_mixer_gain,
        widened(gate_in_wide, gate_in_matrix),
        widened(state_in_sum[:, :, :state_width], state_in_matrix),
        grad_mixer_input_kernel,
        grad_state_conv_kernel,
        grad_step_offset_bias,
        grad_log_decay,
        grad_head_skip,
        grad_gated_gain,
        widened(out_full, mixer_out_matrix),
    )


def solution(mesh):
    tokens = P("dp", "col")
    spread = ("row", "col")
    return jax.shard_map(
        body,
        mesh=mesh,
        in_specs=(
            tokens,
            tokens,
            P("dp"),
            P("dp"),
            P(None, "col"),
            P(None, None, "col", "row"),
            P("row", None, "col"),
            P(None, "col"),
            P(None, None, "col", "row"),
            P(None, "col", None),
            P(None, None, spread),
            P("row", None, "col"),
            P(None, "col", None),
            P("col"),
            P(None, "col", "row"),
            P("col", None),
            P(None, spread),
            P(),
            P(spread),
            P(spread),
            P(spread),
            P(spread),
            P("row", "col"),
            tokens,
        ),
        out_specs=(
            tokens,
            tokens,
            tokens,
            P(None, "col"),
            P(None, None, "col", "row"),
            P("row", None, "col"),
            P(None, "col"),
            P(None, None, "col", "row"),
            P(None, "col", None),
            P(None, None, spread),
            P("row", None, "col"),
            P(None, "col", None),
            P("col"),
            P(None, "col", "row"),
            P("col", None),
            P(None, spread),
            P(),
            P(spread),
            P(spread),
            P(spread),
            P(spread),
            P("row", "col"),
        ),
        check_vma=False,
    )
```

```python
import functools
import math

import jax
import jax.numpy as jnp
from jax import lax
from jax.experimental import pallas as pl
from jax.experimental.pallas import tpu as pltpu
from jax.sharding import PartitionSpec as P

EPS = 1e-05
BF = jnp.bfloat16
F32 = jnp.float32
MESH = pl.DeviceIdType.MESH


def matrix_product(left, right):
    return jnp.dot(left, right, preferred_element_type=F32)


def matmul_tn(left, right):
    return lax.dot_general(left, right, (((0,), (0,)), ((), ())), preferred_element_type=F32)


def matrix_product_transposed(left, right):
    return lax.dot_general(left, right, (((1,), (1,)), ((), ())), preferred_element_type=F32)


def rope_tables(length, width):
    half = width // 2
    positions = jnp.arange(length).astype(F32)
    rates = jnp.exp(-math.log(10000.0) * jnp.arange(half).astype(F32) / half)
    angles = positions[:, None] * rates[None, :]
    cosine, sine = jnp.cos(angles), jnp.sin(angles)
    return jnp.concatenate([cosine, cosine], 1), jnp.concatenate([-sine, sine], 1)


def _dot(left, right, dims=((1,), (0,))):
    return lax.dot_general(left, right, (dims, ((), ())), preferred_element_type=F32)


def _split(value):
    high = value.astype(BF)
    return high, (value - high.astype(F32)).astype(BF)


def _head_weights(q, k, cosine, sine, allowed):
    width = q.shape[1]
    q = q * cosine + pltpu.roll(q, width // 2, 1) * sine
    k = k * cosine + pltpu.roll(k, width // 2, 1) * sine
    q_high, q_low = _split(q)
    k_high, k_low = _split(k)
    rows = ((1,), (1,))
    scores = _dot(q_high, k_high, rows) + _dot(q_high, k_low, rows) + _dot(q_low, k_high, rows)
    weights = jnp.where(allowed, jnp.exp(scores / math.sqrt(width)), 0.0)
    return weights / jnp.sum(weights, -1, keepdims=True), q_high, k_high


def _allowed(seg_col, seg_row):
    length = seg_col.shape[0]
    first = lax.broadcasted_iota(jnp.int32, (length, length), 0)
    second = lax.broadcasted_iota(jnp.int32, (length, length), 1)
    return (first >= second) & (seg_col[...] == seg_row[...])


def attention_forward(qkv, cosine, sine, seg_col, seg_row, o):
    width = cosine.shape[1]
    allowed = _allowed(seg_col, seg_row)
    for head in range(qkv.shape[2] // width):
        part = pl.ds(head * width, width)
        weights, _, _ = _head_weights(
            qkv[0, :, part], qkv[1, :, part], cosine[...], sine[...], allowed
        )
        o[:, part] = _dot(weights.astype(BF), qkv[2, :, part].astype(BF)).astype(BF)


def attention_backward(qkv, cosine, sine, seg_col, seg_row, grad, d_qkv):
    width = cosine.shape[1]
    allowed = _allowed(seg_col, seg_row)
    factor = 1.0 / math.sqrt(width)
    for head in range(qkv.shape[2] // width):
        part = pl.ds(head * width, width)
        weights, q_turned, k_turned = _head_weights(
            qkv[0, :, part], qkv[1, :, part], cosine[...], sine[...], allowed
        )
        grad_b = grad[:, part].astype(BF)
        d_weights = _dot(grad_b, qkv[2, :, part].astype(BF), ((1,), (1,)))
        inner = jnp.sum(d_weights * weights, -1, keepdims=True)
        d_scores = (weights * (d_weights - inner) * factor).astype(BF)
        d_turned = (
            _dot(d_scores, k_turned),
            _dot(d_scores, q_turned, ((0,), (0,))),
        )
        for i in range(2):
            d = d_turned[i]
            d = d * cosine[...] + pltpu.roll(d * sine[...], width // 2, 1)
            d_qkv[i, :, part] = d.astype(BF)
        d_qkv[2, :, part] = _dot(weights.astype(BF), grad_b, ((0,), (0,))).astype(BF)


def local_call(kernel, out_shape, *operands):
    vmem = pl.BlockSpec(memory_space=pltpu.VMEM)
    return pl.pallas_call(
        kernel,
        out_shape=out_shape,
        in_specs=[vmem] * len(operands),
        out_specs=jax.tree.map(lambda _: vmem, out_shape),
        name=kernel.__name__,
    )(*operands)


def conv_causal(signal, kernel, docs):
    total = signal * kernel[0]
    for offset in range(1, kernel.shape[0]):
        shifted = jnp.concatenate(
            [jnp.zeros((offset, signal.shape[1]), signal.dtype), signal[:-offset]], 0
        )
        shifted_docs = jnp.concatenate([jnp.full((offset,), -1, jnp.int32), docs[:-offset]], 0)
        same = (shifted_docs == docs).astype(signal.dtype)[:, None]
        total = total + shifted * kernel[offset] * same
    return total


def bc_activate(bc_pre, kernel, docs):
    return jax.nn.silu(conv_causal(bc_pre, kernel, docs))


def _decay(cum, cum_rows, head, allowed):
    gaps = cum[:, head : head + 1] - cum_rows[head : head + 1, :]
    return jnp.where(allowed, jnp.exp(jnp.where(allowed, gaps, 0.0)), 0.0)


def _thirds(value):
    high, rest = _split(value)
    rest = value - high.astype(F32)
    middle, low = _split(rest)
    return high, middle, low


def _triangle(length):
    first = lax.broadcasted_iota(jnp.int32, (length, length), 0)
    second = lax.broadcasted_iota(jnp.int32, (length, length), 1)
    return (first >= second).astype(F32).astype(BF)


def _running_sums(rate):
    lower = _triangle(rate.shape[0])
    parts = _thirds(rate)
    columns = sum(_dot(lower, part) for part in parts)
    rows = sum(_dot(part, lower, ((0,), (1,))) for part in parts)
    return columns, rows


def _intersection(bc):
    state = bc.shape[1] // 2
    b_high, b_low = _split(bc[:, :state])
    c_high, c_low = _split(bc[:, state:])
    rows = ((1,), (1,))
    total = _dot(c_high, b_high, rows) + _dot(c_high, b_low, rows) + _dot(c_low, b_high, rows)
    return total, b_high, c_high


def mixing_forward(bc, rate, weighted, doc_col, doc_row, o):
    heads = rate.shape[1]
    cum, cum_rows = _running_sums(rate[...])
    width = weighted.shape[1] // heads
    allowed = _allowed(doc_col, doc_row)
    intersection, _, _ = _intersection(bc[...])
    results = []
    for head in range(heads):
        mixing = _decay(cum, cum_rows, head, allowed) * intersection
        part = weighted[:, head * width : (head + 1) * width]
        results.append(_dot(mixing.astype(BF), part.astype(BF)))
    o[...] = jnp.concatenate(results, 1)


def mixing_backward(
    bc, rate, weighted, doc_col, doc_row, grad, d_bc, d_rate, d_weighted
):
    heads = rate.shape[1]
    cum, cum_rows = _running_sums(rate[...])
    lower = _triangle(rate.shape[0])
    width = weighted.shape[1] // heads
    allowed = _allowed(doc_col, doc_row)
    intersection, b, c = _intersection(bc[...])
    d_intersection = jnp.zeros_like(intersection)
    d_parts, ahead, behind = [], [], []
    for head in range(heads):
        decay = _decay(cum, cum_rows, head, allowed)
        mixing = decay * intersection
        part = weighted[:, head * width : (head + 1) * width].astype(BF)
        grad_part = grad[:, head * width : (head + 1) * width].astype(BF)
        d_parts.append(_dot(mixing.astype(BF), grad_part, ((0,), (0,))))
        d_mixing = _dot(grad_part, part, ((1,), (1,)))
        d_intersection = d_intersection + d_mixing * decay
        d_gaps = d_mixing * mixing
        ahead.append(jnp.sum(d_gaps, 1, keepdims=True))
        behind.append(jnp.sum(d_gaps, 0, keepdims=True))
    d_weighted[...] = jnp.concatenate(d_parts, 1)
    columns = sum(
        _dot(lower, part, ((0,), (0,))) for part in _thirds(jnp.concatenate(ahead, 1))
    )
    rows = sum(
        _dot(lower, part, ((0,), (1,))) for part in _thirds(jnp.concatenate(behind, 0))
    )
    d_rate[...] = columns - rows
    d_b = d_intersection.astype(BF)
    d_bc[...] = jnp.concatenate([_dot(d_b, c, ((0,), (0,))), _dot(d_b, b)], 1)


@jax.custom_vjp
def mixing_sum(bc, rate, weighted, doc_col, doc_row):
    shape = jax.ShapeDtypeStruct(weighted.shape, F32)
    return local_call(mixing_forward, shape, bc, rate, weighted, doc_col, doc_row)


def mixing_sum_forward(*operands):
    return mixing_sum(*operands), operands


def mixing_sum_backward(operands, grad):
    shapes = [jax.ShapeDtypeStruct(operand.shape, F32) for operand in operands[:3]]
    d_bc, d_rate, d_weighted = local_call(mixing_backward, shapes, *operands, grad)
    return d_bc, d_rate, d_weighted, None, None


mixing_sum.defvjp(mixing_sum_forward, mixing_sum_backward)


def mixer_core(
    x_pre,
    gate_z,
    step_raw,
    bc_conv,
    conv_kernel,
    step_offset_bias,
    log_decay_rates,
    head_skip_term,
    docs,
):
    length = x_pre.shape[0]
    heads = step_raw.shape[1]
    head_dim = x_pre.shape[1] // heads
    inner = jax.nn.silu(conv_causal(x_pre, conv_kernel, docs)).reshape(length, heads, head_dim)
    step = jax.nn.softplus(step_raw + step_offset_bias)
    rate = -jnp.exp(log_decay_rates) * step
    weighted = (inner * step[:, :, None]).reshape(length, -1)
    outputs = mixing_sum(
        bc_conv, rate, weighted, docs.reshape(length, 1), docs.reshape(1, length)
    ).reshape(inner.shape)
    outputs = outputs + head_skip_term[None, :, None] * inner
    return outputs.reshape(length, heads * head_dim) * jax.nn.silu(gate_z)


def gelu_product(gate_preact, up_preact):
    return jax.nn.gelu(gate_preact, approximate=True) * up_preact


def _window(index, size):
    return pl.ds(pl.multiple_of(index * size, size), size)


def _add_rows(rows, write):
    chunk = 64 if rows % 64 == 0 else rows
    if rows == chunk:
        write(pl.ds(0, rows))
        return

    def step(i, carry):
        write(pl.ds(pl.multiple_of(i * chunk, chunk), chunk))
        return carry

    lax.fori_loop(0, rows // chunk, step, 0)


def _remote(src, dst, send, recv, device):
    copy = pltpu.make_async_remote_copy(
        src_ref=src,
        dst_ref=dst,
        send_sem=send,
        recv_sem=recv,
        device_id=device,
        device_id_type=MESH,
    )
    copy.start()
    return copy


class Env:
    def __init__(self, n, replicas):
        self.n = n
        self.replicas = replicas
        self.dp = lax.axis_index("dp")
        self.col = lax.axis_index("col")
        self.row = lax.axis_index("row")
        self.sibling = {"row": 1 - self.row}

    def peer(self, k):
        return {"col": lax.rem(self.col + k, self.n)}

    def replica(self, k):
        return {"dp": lax.rem(self.dp + k, self.replicas)}


class Relay:

    def __init__(self, env, where, send, recv, direction):
        self.env, self.where, self.direction = env, where, direction
        self.send, self.recv = send, recv
        self.base = 0 if direction > 0 else env.n - 1
        self.neighbour = {"col": jnp.clip(env.col + direction, 0, env.n - 1)}

    def copy(self, step, source):
        i = self.base + step
        return pltpu.make_async_remote_copy(
            src_ref=source,
            dst_ref=self.where(self.owner(step)),
            send_sem=self.send.at[i],
            recv_sem=self.recv.at[i],
            device_id=self.neighbour,
            device_id_type=MESH,
        )

    def owner(self, step):
        owner = self.env.col - self.direction * step
        return jnp.clip(owner, 0, self.env.n - 1)

    def place(self):
        return self.env.col if self.direction > 0 else self.env.n - 1 - self.env.col

    def sends(self, step):
        return (self.place() < self.env.n - 1) & (self.place() >= step)

    def receives(self, step):
        return self.place() > step

    def start(self, step, source):
        @pl.when(self.sends(step))
        def _():
            self.copy(step, source).start()

    def arrived(self, step, then=None):
        @pl.when(self.receives(step))
        def _():
            part = self.where(self.owner(step + 1))
            pltpu.make_async_remote_copy(
                src_ref=part,
                dst_ref=part,
                send_sem=self.send.at[self.base + step],
                recv_sem=self.recv.at[self.base + step],
                device_id=self.neighbour,
                device_id_type=MESH,
            ).wait_recv()
            if then is not None:
                then(part, self.base + step)

    def sent(self, step, source):
        @pl.when(self.sends(step))
        def _():
            self.copy(step, source).wait_send()


def run_gather(env, x, o, send, recv, local):
    width = x.shape[1]

    def where(owner):
        return o.at[:, _window(owner, width)]

    own = pltpu.make_async_copy(x, where(env.col), local.at[0])
    ways = [Relay(env, where, send, recv, d) for d in (1, -1)]
    for way in ways:
        way.start(0, x)
    own.start()
    yield
    for step in range(env.n - 1):
        for way in ways:
            way.arrived(step)
            if step < env.n - 2:
                way.start(step + 1, where(way.owner(step + 1)))
        yield
    own.wait()
    for step in range(env.n - 1):
        for way in ways:
            way.sent(step, x)


def run_gather2(env, x, o, send, recv, local, send2, recv2):
    width = x.shape[1]
    half = x.shape[0] // 2
    mine = _window(env.row, half)

    def where(owner):
        return o.at[mine, _window(owner, width)]

    source = x.at[mine, :]

    def across(part, i):
        return pltpu.make_async_remote_copy(
            src_ref=part,
            dst_ref=part,
            send_sem=send2.at[i],
            recv_sem=recv2.at[i],
            device_id=env.sibling,
            device_id_type=MESH,
        )

    def pass_on(part, i):
        across(part, i).start()

    own = pltpu.make_async_copy(x, o.at[:, _window(env.col, width)], local.at[0])
    ways = [Relay(env, where, send, recv, d) for d in (1, -1)]
    for way in ways:
        way.start(0, source)
    own.start()
    yield
    for step in range(env.n - 1):
        for way in ways:
            way.arrived(step, pass_on)
            if step < env.n - 2:
                way.start(step + 1, where(way.owner(step + 1)))
        yield
    own.wait()
    for step in range(env.n - 1):
        for way in ways:
            way.sent(step, source)

            @pl.when(way.receives(step))
            def _(way=way, step=step):
                part = where(way.owner(step + 1))
                across(part, way.base + step).wait()


def run_scatter(env, p, o, buffer, send, recv):
    rows, width = o.shape
    copies = [
        _remote(
            p.at[:, _window(lax.rem(env.col + k, env.n), width)],
            buffer.at[k - 1],
            send.at[k - 1],
            recv.at[k - 1],
            env.peer(k),
        )
        for k in range(1, env.n)
    ]
    yield
    for copy in copies:
        copy.wait()

    def write(part):
        total = p[part, _window(env.col, width)].astype(F32)
        for k in range(env.n - 1):
            total = total + buffer[k, part, :].astype(F32)
        o[part, :] = total

    _add_rows(rows, write)


def run_scatter2(env, p, o, buffer, send, recv, send2, recv2):
    rows, width = p.shape[0], o.shape[1]
    size = rows // 2
    copies = []
    for c in range(2):
        for k in range(1, env.n):
            i = c * (env.n - 1) + k - 1
            part = pl.ds(c * size, size)
            copies.append(
                _remote(
                    p.at[part, _window(lax.rem(env.col + k, env.n), width)],
                    buffer.at[k - 1, part, :],
                    send.at[i],
                    recv.at[i],
                    env.peer(k),
                )
            )
    yield
    first = env.row * rows
    onward = []
    for c in range(2):
        for k in range(1, env.n):
            copies[c * (env.n - 1) + k - 1].wait()

        def write(part, c=c):
            source = pl.ds(pl.multiple_of(c * size + part.start, 16), part.size)
            total = p[source, _window(env.col, width)].astype(F32)
            for k in range(env.n - 1):
                total = total + buffer[k, source, :].astype(F32)
            target = pl.ds(pl.multiple_of(first + c * size + part.start, 8), part.size)
            o[target, :] = total

        _add_rows(size, write)
        half = o.at[_window(env.row * 2 + c, size), :]
        onward.append(_remote(half, half, send2.at[c], recv2.at[c], env.sibling))
    yield
    for copy in onward:
        copy.wait()


def run_reduce(env, p, o, pairs, sums, buffer, send, recv, send2, recv2, send3, recv3):
    rows, width = o.shape
    half = rows // 2
    size = half // 2
    other = _window(1 - env.row, half)
    order = [(k + 1) % env.n for k in range(env.n)]
    first = []
    for i, k in enumerate(order):
        piece = _window(lax.rem(env.col + k, env.n), width)
        first.append(
            _remote(p.at[other, piece], pairs.at[i], send.at[i], recv.at[i], env.sibling)
        )
    yield
    start = env.row * half
    copies = {}
    for i, k in enumerate(order):
        first[i].wait()
        piece = _window(lax.rem(env.col + k, env.n), width)

        def write(part, i=i, piece=piece):
            source = pl.ds(pl.multiple_of(start + part.start, 16), part.size)
            total = p[source, piece].astype(F32) + pairs[i, part, :].astype(F32)
            sums[i, part, :] = total.astype(sums.dtype)

        _add_rows(half, write)
        if k:
            for c in range(2):
                part = pl.ds(c * size, size)
                j = 2 * i + c
                copies[j] = _remote(
                    sums.at[i, part, :],
                    buffer.at[i, part, :],
                    send2.at[j],
                    recv2.at[j],
                    env.peer(k),
                )
    yield
    onward = []
    for c in range(2):
        for i in range(env.n - 1):
            copies[2 * i + c].wait()

        def finish(part, c=c):
            source = pl.ds(pl.multiple_of(c * size + part.start, 16), part.size)
            total = sums[env.n - 1, source, :].astype(F32)
            for k in range(env.n - 1):
                total = total + buffer[k, source, :].astype(F32)
            target = pl.ds(pl.multiple_of(start + c * size + part.start, 8), part.size)
            o[target, :] = total

        _add_rows(size, finish)
        part = o.at[_window(env.row * 2 + c, size), :]
        onward.append(_remote(part, part, send3.at[c], recv3.at[c], env.sibling))
    yield
    for copy in onward:
        copy.wait()


def run_a2a(env, x, o, send, recv, local):
    for _ in range(env.n - 2):
        yield
    width = o.shape[3]
    copies = [
        _remote(
            x.at[:, :, _window(lax.rem(env.col + k, env.n), width)],
            o.at[:, env.col],
            send.at[k - 1],
            recv.at[k - 1],
            env.peer(k),
        )
        for k in range(1, env.n)
    ]
    own = pltpu.make_async_copy(
        x.at[:, :, _window(env.col, width)], o.at[:, env.col], local.at[0]
    )
    own.start()
    yield
    own.wait()
    for copy in copies:
        copy.wait()


def run_a2a_back(delay, env, x, o, send, recv, local):
    for _ in range(delay):
        yield
    here = o.at[:, :, _window(env.col, x.shape[3])]
    copies = [
        _remote(
            x.at[:, lax.rem(env.col + k, env.n)],
            here,
            send.at[k - 1],
            recv.at[k - 1],
            env.peer(k),
        )
        for k in range(1, env.n)
    ]
    own = pltpu.make_async_copy(x.at[:, env.col], here, local.at[0])
    own.start()
    yield
    own.wait()
    for copy in copies:
        copy.wait()


def run_dpscatter(env, x, o, buffer, send, recv):
    groups, rows, _ = o.shape
    copies = [
        _remote(
            x.at[:, _window(lax.rem(env.dp + k, env.replicas), rows), :],
            buffer.at[k - 1],
            send.at[k - 1],
            recv.at[k - 1],
            env.replica(k),
        )
        for k in range(1, env.replicas)
    ]
    yield
    for copy in copies:
        copy.wait()
    start = env.dp * rows
    chunk = 64 if rows % 64 == 0 else rows
    steps = rows // chunk

    def step(i, carry):
        group = i // steps
        first = (i % steps) * chunk
        source = pl.ds(pl.multiple_of(start + first, 16), chunk)
        part = pl.ds(pl.multiple_of(first, 16), chunk)
        total = x[group, source, :].astype(F32)
        for k in range(env.replicas - 1):
            total = total + buffer[k, group, part, :].astype(F32)
        o[group, part, :] = total.astype(o.dtype)
        return carry

    lax.fori_loop(0, groups * steps, step, 0)


def run_dpgather(env, x, o, send, recv, local):
    here = o.at[:, _window(env.dp, x.shape[1]), :]
    copies = [
        _remote(x, here, send.at[k - 1], recv.at[k - 1], env.replica(k))
        for k in range(1, env.replicas)
    ]
    own = pltpu.make_async_copy(x, here, local.at[0])
    own.start()
    yield
    own.wait()
    for copy in copies:
        copy.wait()


def run_dpsum(env, s, o, buffer, send, recv, local):
    copies = [
        _remote(s, buffer.at[env.dp], send.at[k - 1], recv.at[k - 1], env.replica(k))
        for k in range(1, env.replicas)
    ]
    own = pltpu.make_async_copy(s, buffer.at[env.dp], local.at[0])
    own.start()
    yield
    own.wait()
    for copy in copies:
        copy.wait()
    total = buffer[0]
    for i in range(1, env.replicas):
        total = total + buffer[i]
    o[...] = total


def run_rowsum(env, p, o, buffer, send, recv):
    copy = _remote(p, buffer, send.at[0], recv.at[0], env.sibling)
    yield
    copy.wait()

    def write(part):
        o[part, :] = p[part, :].astype(F32) + buffer[part, :].astype(F32)

    _add_rows(p.shape[0], write)


def run_sum(env, s, o, buffer, send, recv, local):
    both = buffer.shape[0] > env.n
    mine = env.row * env.n + env.col if both else env.col
    copies = []
    for r in range(2 if both else 1):
        for k in range(env.n):
            if r == 0 and k == 0:
                continue
            device = dict(env.peer(k)) if k else {}
            if r:
                device["row"] = 1 - env.row
            index = r * env.n + k - 1
            copies.append(_remote(s, buffer.at[mine], send.at[index], recv.at[index], device))
    own = pltpu.make_async_copy(s, buffer.at[mine], local.at[0])
    own.start()
    yield
    own.wait()
    for copy in copies:
        copy.wait()
    total = buffer[0]
    for i in range(1, buffer.shape[0]):
        total = total + buffer[i]
    o[...] = total


def plan(kind, x, n, replicas):
    dma = pltpu.SemaphoreType.DMA
    shape = x.shape
    three = dma((n - 1,))
    one, two = dma((1,)), dma((2,))
    twice = dma((2 * (n - 1),))
    if kind == "gather":
        return run_gather, (shape[0], n * shape[1]), x.dtype, [twice, twice, one]
    if kind == "gather2":
        scratch = [twice, twice, one, twice, twice]
        return run_gather2, (shape[0], n * shape[1]), x.dtype, scratch
    if kind == "scatter":
        out = (shape[0], shape[1] // n)
        return run_scatter, out, F32, [pltpu.VMEM((n - 1,) + out, x.dtype), three, three]
    if kind == "scatter2":
        part = (shape[0], shape[1] // n)
        out = (2 * shape[0], shape[1] // n)
        scratch = [pltpu.VMEM((n - 1,) + part, x.dtype), twice, twice, two, two]
        return run_scatter2, out, F32, scratch
    if kind == "reduce":
        out = (shape[0], shape[1] // n)
        part = (shape[0] // 2, shape[1] // n)
        four = dma((n,))
        scratch = [
            pltpu.VMEM((n,) + part, x.dtype),
            pltpu.VMEM((n,) + part, x.dtype),
            pltpu.VMEM((n - 1,) + part, x.dtype),
            four,
            four,
            twice,
            twice,
            two,
            two,
        ]
        return run_reduce, out, F32, scratch
    if kind == "a2a":
        return run_a2a, (shape[0], n, shape[1], shape[2] // n), x.dtype, [three, three, one]
    if kind.startswith("a2a_back"):
        delay = {"a2a_back": 0, "a2a_back1": 1, "a2a_back2": n - 2}[kind]
        run = functools.partial(run_a2a_back, delay)
        return run, (shape[0], shape[2], n * shape[3]), x.dtype, [three, three, one]
    if kind.startswith("dp"):
        others = dma((replicas - 1,))
        if kind == "dpscatter":
            out = (shape[0], shape[1] // replicas, shape[2])
            return run_dpscatter, out, x.dtype, [
                pltpu.VMEM((replicas - 1,) + out, x.dtype),
                others,
                others,
            ]
        if kind == "dpgather":
            out = (shape[0], shape[1] * replicas, shape[2])
            return run_dpgather, out, x.dtype, [others, others, one]
        scratch = [pltpu.VMEM((replicas,) + shape, x.dtype), others, others, one]
        return run_dpsum, shape, F32, scratch
    if kind == "rowsum":
        return run_rowsum, shape, F32, [pltpu.VMEM(shape, x.dtype), one, one]
    members = n if kind == "colsum" else 2 * n
    many = dma((members - 1,))
    return run_sum, shape, F32, [pltpu.VMEM((members,) + shape, x.dtype), many, many, one]


def exchange(ident, items, micros):
    n = lax.axis_size("col")
    replicas = lax.axis_size("dp")
    plans = [plan(kind, x, n, replicas) for kind, x in items]
    kinds = {kind for kind, _ in items}
    count = len(items)
    use_all = "allsum" in kinds
    use_dp = any(kind.startswith("dp") for kind in kinds)
    use_col = use_all or any(kind != "rowsum" and not kind.startswith("dp") for kind in kinds)
    use_row = use_all or bool(kinds & {"rowsum", "gather2", "scatter2", "reduce"})

    def kernel(*refs):
        env = Env(n, replicas)
        barrier = pltpu.get_barrier_semaphore()
        targets = []
        if use_col:
            targets += [env.peer(k) for k in range(1, n)]
        if use_row:
            targets.append(env.sibling)
        if use_all:
            targets += [{**env.peer(k), **env.sibling} for k in range(1, n)]
        if use_dp:
            targets += [env.replica(k) for k in range(1, replicas)]
        for target in targets:
            pl.semaphore_signal(barrier, inc=1, device_id=target, device_id_type=MESH)
        pl.semaphore_wait(barrier, len(targets))
        position = 2 * count
        running = []
        for i in range(count):
            size = len(plans[i][3])
            scratch = refs[position : position + size]
            position += size
            running.append(plans[i][0](env, refs[i], refs[count + i], *scratch))
        while running:
            alive = []
            for item in running:
                try:
                    next(item)
                except StopIteration:
                    continue
                alive.append(item)
            running = alive

    vmem = pl.BlockSpec(memory_space=pltpu.VMEM)
    return pl.pallas_call(
        kernel,
        out_shape=[jax.ShapeDtypeStruct(p[1], p[2]) for p in plans],
        in_specs=[vmem] * count,
        out_specs=[vmem] * count,
        scratch_shapes=[s for p in plans for s in p[3]],
        compiler_params=pltpu.CompilerParams(collective_id=ident, has_side_effects=True),
        cost_estimate=pl.CostEstimate(
            flops=0, bytes_accessed=int(micros * 3000000), transcendentals=0
        ),
        name="exchange_%d" % ident,
    )(*[x for _, x in items])


def pack_rows(*vectors):
    return jnp.concatenate([v.reshape(-1, 128) for v in vectors], 0)


def unpack_rows(packed, count):
    return [part.reshape(-1) for part in jnp.split(packed, count, 0)]


def body(
    hidden_state_input,
    initial_token_embedding,
    document_numbers,
    document_start_flags,
    attention_norm_gain,
    query_key_value_matrix,
    attention_out_matrix,
    perceptron_norm_gain,
    gate_up_matrix,
    adapter_down,
    adapter_up,
    down_matrix,
    projection_matrix,
    mixer_norm_gain,
    gate_in_matrix,
    state_in_matrix,
    mixer_input_kernel,
    state_conv_kernel,
    step_offset_bias,
    log_decay_rates,
    head_skip_term,
    gated_norm_gain,
    mixer_out_matrix,
    output_gradient,
):
    n = lax.axis_size("col")
    replicas = lax.axis_size("dp")
    dp, row, col = lax.axis_index("dp"), lax.axis_index("row"), lax.axis_index("col")
    length, width = hidden_state_input.shape
    local_width = 2 * width
    model_width = n * width
    concat_width = n * local_width
    inner_width = gated_norm_gain.shape[0] * 2 * n

    def my_rows(weight):
        share = weight.shape[2] // replicas
        part = lax.dynamic_slice_in_dim(weight, dp * share, share, 2)
        return part.reshape(weight.shape[0], -1, weight.shape[3])

    def spread(pieces, inner):
        outer, own = pieces.shape[0], pieces.shape[3]
        shaped = pieces.reshape(outer, n, inner, -1, own)
        full = lax.all_gather(shaped, "dp", axis=3, tiled=True)
        return full.reshape(outer, -1, own)

    def after(value, *others):
        return lax.optimization_barrier((value,) + others)[0]

    attn_gain = attention_norm_gain.reshape(local_width)
    mlp_gain = perceptron_norm_gain.reshape(local_width)
    attn_out_flat = attention_out_matrix.reshape(attention_out_matrix.shape[0], local_width)
    down_flat = down_matrix.reshape(down_matrix.shape[0], local_width)
    proj_flat = projection_matrix.reshape(local_width, projection_matrix.shape[2])
    adapter_up_broad = adapter_up.astype(F32)
    state_width = state_in_matrix.shape[1]
    state_pad = jnp.pad(state_in_matrix, ((0, 0), (0, -state_width % 128)))

    (qkv_pieces,) = exchange(0, [("a2a", my_rows(query_key_value_matrix))], 20)
    qkv_t = spread(qkv_pieces, 2)

    concat = (
        jnp.stack([hidden_state_input, initial_token_embedding], 1)
        .astype(F32)
        .reshape(length, local_width)
    )
    x_one, sum_one, gate_up_pieces, gate_in_pieces, adapter_down_full, state_full = exchange(
        1,
        [
            ("gather2", after((concat * attn_gain).astype(BF), qkv_pieces)),
            ("colsum", pack_rows(jnp.sum(concat * concat, 1))),
            ("a2a", my_rows(gate_up_matrix)),
            ("a2a", my_rows(gate_in_matrix[:, None])),
            ("gather2", adapter_down.reshape(local_width, -1)),
            ("gather2", state_pad),
        ],
        60,
    )

    gate_up_t = spread(after(gate_up_pieces, qkv_t), 2)
    gate_in_t = spread(after(gate_in_pieces, gate_up_t), 1)

    def stacked(gathered, lanes):
        rows = gathered.shape[0]
        return gathered.reshape(rows, n, lanes).transpose(1, 0, 2).reshape(n * rows, lanes)

    down_full = stacked(adapter_down_full, adapter_down.shape[2])
    state_in_full = stacked(state_full, state_pad.shape[1])[:, :state_width]

    d_normed_four = lax.psum_scatter(
        matrix_product_transposed(output_gradient, mixer_out_matrix).astype(BF)[None],
        "col",
        scatter_dimension=2,
        tiled=True,
    )[0].astype(F32)

    scale_one = lax.rsqrt(sum_one.reshape(-1) / concat_width + EPS)[:, None]
    norm_one = concat * scale_one
    normed_one = (x_one.astype(F32) * scale_one).astype(BF)
    head_size = 128
    qkv_own = jnp.einsum("tk,iko->ito", normed_one, qkv_t, preferred_element_type=F32)
    shared_tables = (
        *rope_tables(length, head_size),
        document_numbers.reshape(length, 1),
        document_numbers.reshape(1, length),
    )
    attended = local_call(
        attention_forward,
        jax.ShapeDtypeStruct((length, qkv_own.shape[2]), BF),
        qkv_own,
        *shared_tables,
    )
    (heads_half,) = exchange(2, [("gather", attended)], 25)
    (attn_sum,) = exchange(
        3, [("rowsum", matrix_product(heads_half, attn_out_flat).astype(BF))], 5
    )
    attn_stream = concat + attn_sum
    x_two, sum_two = exchange(
        4,
        [
            ("gather2", (attn_stream * mlp_gain).astype(BF)),
            ("colsum", pack_rows(jnp.sum(attn_stream * attn_stream, 1))),
        ],
        25,
    )
    scale_two = lax.rsqrt(sum_two.reshape(-1) / concat_width + EPS)[:, None]
    norm_two = attn_stream * scale_two
    normed_two = (x_two.astype(F32) * scale_two).astype(BF)
    adapter_middle = matrix_product(normed_two, down_full)
    gate_up_local = jnp.einsum("tk,iko->ito", normed_two, gate_up_t, preferred_element_type=F32)
    gate_up_local = gate_up_local + jnp.einsum(
        "gb,sbm->sgm", adapter_middle, adapter_up_broad
    )
    hidden_own = gelu_product(gate_up_local[0], gate_up_local[1]).astype(BF)
    (hidden_half,) = exchange(5, [("gather", hidden_own)], 45)
    (mlp_sum,) = exchange(6, [("rowsum", matrix_product(hidden_half, down_flat).astype(BF))], 5)
    mixed_b = (attn_stream + mlp_sum).astype(BF)
    half_tokens = lax.dynamic_slice_in_dim(mixed_b, row * (length // 2), length // 2, 0)
    (proj_sum,) = exchange(7, [("scatter2", matrix_product(half_tokens, proj_flat).astype(BF))], 15)
    resid = hidden_state_input.astype(F32) + proj_sum
    x_three, sum_three = exchange(
        8,
        [
            ("gather2", (resid * mixer_norm_gain).astype(BF)),
            ("colsum", pack_rows(jnp.sum(resid * resid, 1))),
        ],
        15,
    )
    scale_three = lax.rsqrt(sum_three.reshape(-1) / model_width + EPS)[:, None]
    norm_three = resid * scale_three
    normed_three = (x_three.astype(F32) * scale_three).astype(BF)
    zx_own = jnp.einsum("tk,iko->ito", normed_three, gate_in_t, preferred_element_type=F32)
    bcdt = matrix_product(normed_three, state_in_full)
    state_cols = state_conv_kernel.shape[1]
    heads_own = step_offset_bias.shape[0]
    owner = row * n + col
    step_own = lax.dynamic_slice_in_dim(bcdt, state_cols + owner * heads_own, heads_own, 1)
    docs = jnp.cumsum(document_start_flags) - 1
    bc_conv, bc_back = jax.vjp(
        functools.partial(bc_activate, docs=docs), bcdt[:, :state_cols], state_conv_kernel
    )
    gated, core_back = jax.vjp(
        functools.partial(mixer_core, docs=docs),
        zx_own[1],
        zx_own[0],
        step_own,
        bc_conv,
        mixer_input_kernel,
        step_offset_bias,
        log_decay_rates,
        head_skip_term,
    )
    grad_hat = d_normed_four * gated_norm_gain
    (sums_four,) = exchange(
        9,
        [("allsum", pack_rows(jnp.sum(gated * gated, 1), jnp.sum(grad_hat * gated, 1)))],
        6,
    )
    square_four, cross_four = unpack_rows(sums_four, 2)
    scale_four = lax.rsqrt(square_four / inner_width + EPS)[:, None]
    norm_four = gated * scale_four
    inner_four = cross_four[:, None] * scale_four / inner_width
    d_gated = scale_four * (grad_hat - norm_four * inner_four)
    grad_gated_gain = jnp.sum(d_normed_four * norm_four, 0)
    normed_half = lax.all_gather(
        (norm_four * gated_norm_gain).astype(BF)[None], "col", axis=2, tiled=True
    )[0]

    (
        d_x_pre,
        d_gate_z,
        d_step_own,
        d_bc_part,
        grad_mixer_input_kernel,
        grad_step_offset_bias,
        grad_log_decay,
        grad_head_skip,
    ) = core_back(d_gated)
    step_slot = lax.dynamic_update_slice_in_dim(
        jnp.zeros((length, state_width - state_cols), F32), d_step_own, owner * heads_own, 1
    )
    d_bc_pre, grad_state_conv_kernel = bc_back(d_bc_part)
    d_bcdt_b = jnp.concatenate([d_bc_pre, step_slot], 1).astype(BF)
    d_zx_own = jnp.stack([d_gate_z, d_x_pre]).astype(BF)
    partial_three = jnp.einsum(
        "ito,iko->tk", d_zx_own, gate_in_t, preferred_element_type=F32
    ) + matrix_product_transposed(d_bcdt_b, state_in_full)
    cross_three = jnp.sum(d_zx_own.astype(F32) * zx_own, (0, 2)) + jnp.sum(
        d_bcdt_b.astype(F32) * bcdt, 1
    )
    grad_gate_in = jnp.einsum("tk,ito->iko", normed_three, d_zx_own, preferred_element_type=F32)

    def split_features(grad, inner):
        outer, own = grad.shape[0], grad.shape[2]
        return grad.astype(BF).reshape(outer, n, inner, -1, own)

    def grouped(grad, inner):
        groups = split_features(grad, inner)
        return groups.reshape((-1,) + groups.shape[3:])

    def ungrouped(share, outer):
        return share.reshape(outer, n, -1, share.shape[2])

    def share_of(grad, inner):
        share = lax.psum_scatter(
            split_features(grad, inner), "dp", scatter_dimension=3, tiled=True
        )
        return share.reshape(share.shape[0], n, -1, share.shape[4])

    def joined(back, inner):
        shaped = back.reshape(back.shape[0], inner, -1, back.shape[2])
        return lax.all_gather(shaped, "dp", axis=2, tiled=True)

    d_normed_three, inner_three, gate_in_share = exchange(
        10,
        [
            ("reduce", after(partial_three.astype(BF), normed_half)),
            ("allsum", pack_rows(cross_three)),
            ("dpscatter", grouped(grad_gate_in, 1)),
        ],
        25,
    )

    def norm_back(grad_in, inner, normal, scale, gain, count):
        mean = inner.reshape(-1)[:, None] / count
        return scale * (grad_in * gain - normal * mean), jnp.sum(grad_in * normal, 0)

    grad_state_in_part = matmul_tn(normed_three, d_bcdt_b)
    d_norm_three, grad_mixer_gain = norm_back(
        d_normed_three, inner_three, norm_three, scale_three, mixer_norm_gain, model_width
    )
    d_resid = output_gradient.astype(F32) + d_norm_three
    d_resid_full, conv_sum, gate_in_back = exchange(
        11,
        [
            ("gather2", d_resid.astype(BF)),
            ("allsum", grad_state_conv_kernel),
            ("a2a_back2", ungrouped(gate_in_share, 2)),
        ],
        28,
    )
    gate_in_wide = joined(gate_in_back, 1)
    grad_proj = matmul_tn(mixed_b, d_resid_full).astype(BF)
    d_mixed = matrix_product_transposed(d_resid_full, proj_flat)
    d_mixed_b = d_mixed.astype(BF)
    grad_down = matmul_tn(hidden_half, d_mixed_b).astype(BF)
    partial_hidden = matrix_product_transposed(d_mixed_b, down_flat).astype(BF)
    (d_hidden_own,) = exchange(
        12, [("scatter", after(partial_hidden, grad_proj, grad_down))], 50
    )
    proj_full, down_full_grad = lax.psum((grad_proj, grad_down), "dp")
    act_back = jax.vjp(gelu_product, gate_up_local[0], gate_up_local[1])[1]
    grad_gate_up_local = jnp.stack(act_back(d_hidden_own))
    grad_adapter_up = jnp.einsum(
        "mc,ymv->ycv", adapter_middle, grad_gate_up_local
    )
    middle_part = jnp.einsum(
        "oaj,opj->ap", grad_gate_up_local, adapter_up_broad
    ).astype(BF)
    d_gate_up_b = grad_gate_up_local.astype(BF)
    partial_two = jnp.einsum(
        "ito,iko->tk", d_gate_up_b, gate_up_t, preferred_element_type=F32
    ) + matrix_product_transposed(middle_part, down_full)
    cross_two = jnp.sum(d_gate_up_b.astype(F32) * gate_up_local, (0, 2))
    grad_gate_up = jnp.einsum(
        "tk,ito->iko", normed_two, d_gate_up_b, preferred_element_type=F32
    ).astype(BF)
    gate_up_share = share_of(grad_gate_up, 2)
    d_normed_two, inner_two = exchange(
        13,
        [
            ("reduce", after(partial_two.astype(BF), grad_gate_up)),
            ("allsum", pack_rows(cross_two)),
        ],
        30,
    )
    grad_adapter_down_part = matmul_tn(normed_two, middle_part).astype(BF)

    def by_owner(part):
        lanes = part.shape[1] + -part.shape[1] % 128
        padded = jnp.pad(part, ((0, 0), (0, lanes - part.shape[1])))
        return padded.reshape(n, -1, lanes).transpose(1, 0, 2).reshape(-1, n * lanes)
    d_norm_two, grad_perceptron_gain = norm_back(
        d_normed_two, inner_two, norm_two, scale_two, mlp_gain, concat_width
    )
    d_attn = d_mixed + d_norm_two
    d_attn_b = d_attn.astype(BF)
    grad_attention_out = matmul_tn(heads_half, d_attn_b).astype(BF)
    grad_up_flat = grad_adapter_up.astype(BF).reshape(-1, grad_adapter_up.shape[2])
    grad_mixer_out = matmul_tn(after(normed_half, d_normed_two), output_gradient).astype(BF)
    (
        adapter_down_sum,
        state_in_sum,
        gate_up_back,
        out_share,
        attn_out_share,
        up_share,
        d_heads_own,
    ) = exchange(
        14,
        [
            ("reduce", by_owner(grad_adapter_down_part)),
            ("reduce", by_owner(grad_state_in_part.astype(BF))),
            ("a2a_back1", gate_up_share),
            ("dpscatter", grad_mixer_out[None]),
            ("dpscatter", grad_attention_out[None]),
            ("dpscatter", grad_up_flat[None]),
            (
                "scatter",
                after(
                    matrix_product_transposed(d_attn_b, attn_out_flat).astype(BF),
                    proj_full,
                    down_full_grad,
                    gate_in_wide,
                ),
            ),
        ],
        50,
    )
    gate_up_wide = joined(gate_up_back, 2)
    d_qkv_b = local_call(
        attention_backward,
        jax.ShapeDtypeStruct(qkv_own.shape, BF),
        qkv_own,
        *shared_tables,
        d_heads_own,
    )
    partial_one = jnp.einsum("ito,iko->tk", d_qkv_b, qkv_t, preferred_element_type=F32)
    cross_one = jnp.sum(d_qkv_b.astype(F32) * qkv_own, (0, 2))
    grad_qkv = jnp.einsum("tk,ito->iko", normed_one, d_qkv_b, preferred_element_type=F32)
    (
        d_normed_one,
        inner_one,
        qkv_share,
        adapter_down_share,
        state_in_share,
        out_sum,
    ) = exchange(
        15,
        [
            ("reduce", partial_one.astype(BF)),
            ("allsum", pack_rows(cross_one)),
            ("dpscatter", grouped(grad_qkv, 2)),
            ("dpscatter", adapter_down_sum.astype(BF)[None]),
            ("dpscatter", state_in_sum.astype(BF)[None]),
            ("rowsum", matrix_product(after(normed_half, d_normed_two), mixer_out_matrix).astype(BF)),
        ],
        50,
    )
    d_norm_one, grad_attention_gain = norm_back(
        d_normed_one, inner_one, norm_one, scale_one, attn_gain, concat_width
    )
    d_concat = (d_attn + d_norm_one).reshape(length, 2, width)
    grad_hidden = d_resid + d_concat[:, 0]
    grad_embed = d_concat[:, 1]

    small = (
        grad_attention_gain,
        grad_perceptron_gain,
        grad_mixer_gain,
        grad_mixer_input_kernel,
        grad_step_offset_bias,
        grad_log_decay,
        grad_head_skip,
        grad_gated_gain,
        conv_sum,
    )
    flat = jnp.concatenate([value.reshape(-1) for value in small])
    packed = jnp.pad(flat, (0, -flat.size % 1024)).reshape(-1, 128)
    outer = query_key_value_matrix.shape[0]
    (
        qkv_back,
        out_full,
        attn_out_full,
        up_full,
        adapter_down_sum,
        state_in_sum,
        packed_sum,
    ) = exchange(
        16,
        [
            ("a2a_back", ungrouped(qkv_share, outer)),
            ("dpgather", out_share),
            ("dpgather", attn_out_share),
            ("dpgather", up_share),
            ("dpgather", adapter_down_share),
            ("dpgather", state_in_share),
            ("dpsum", packed),
        ],
        20,
    )
    grad_query_key_value = joined(after(qkv_back, gate_up_wide), 2)
    block_out = (resid + after(out_sum, qkv_back)).astype(BF)
    summed, position = [], 0
    for value in small:
        part = packed_sum.reshape(-1)[position : position + value.size]
        summed.append(part.reshape(value.shape))
        position += value.size
    (
        grad_attention_gain,
        grad_perceptron_gain,
        grad_mixer_gain,
        grad_mixer_input_kernel,
        grad_step_offset_bias,
        grad_log_decay,
        grad_head_skip,
        grad_gated_gain,
        grad_state_conv_kernel,
    ) = summed

    def widened(value, like):
        return after(value, qkv_back).astype(F32).reshape(like.shape)

    return (
        block_out,
        grad_hidden,
        grad_embed,
        grad_attention_gain.reshape(attention_norm_gain.shape),
        grad_query_key_value.astype(F32).reshape(query_key_value_matrix.shape),
        widened(attn_out_full, attention_out_matrix),
        grad_perceptron_gain.reshape(perceptron_norm_gain.shape),
        widened(gate_up_wide, gate_up_matrix),
        widened(adapter_down_sum, adapter_down),
        widened(up_full, adapter_up),
        widened(down_full_grad, down_matrix),
        widened(proj_full, projection_matrix),
        grad_mixer_gain,
        widened(gate_in_wide, gate_in_matrix),
        widened(state_in_sum[:, :, :state_width], state_in_matrix),
        grad_mixer_input_kernel,
        grad_state_conv_kernel,
        grad_step_offset_bias,
        grad_log_decay,
        grad_head_skip,
        grad_gated_gain,
        widened(out_full, mixer_out_matrix),
    )


def solution(mesh):
    tokens = P("dp", "col")
    spread = ("row", "col")
    return jax.shard_map(
        body,
        mesh=mesh,
        in_specs=(
            tokens,
            tokens,
            P("dp"),
            P("dp"),
            P(None, "col"),
            P(None, None, "col", "row"),
            P("row", None, "col"),
            P(None, "col"),
            P(None, None, "col", "row"),
            P(None, "col", None),
            P(None, None, spread),
            P("row", None, "col"),
            P(None, "col", None),
            P("col"),
            P(None, "col", "row"),
            P("col", None),
            P(None, spread),
            P(),
            P(spread),
            P(spread),
            P(spread),
            P(spread),
            P("row", "col"),
            tokens,
        ),
        out_specs=(
            tokens,
            tokens,
            tokens,
            P(None, "col"),
            P(None, None, "col", "row"),
            P("row", None, "col"),
            P(None, "col"),
            P(None, None, "col", "row"),
            P(None, "col", None),
            P(None, None, spread),
            P("row", None, "col"),
            P(None, "col", None),
            P("col"),
            P(None, "col", "row"),
            P("col", None),
            P(None, spread),
            P(),
            P(spread),
            P(spread),
            P(spread),
            P(spread),
            P("row", "col"),
        ),
        check_vma=False,
    )
```

```python
import functools
import math

import jax
import jax.numpy as jnp
from jax import lax
from jax.experimental import pallas as pl
from jax.experimental.pallas import tpu as pltpu
from jax.sharding import PartitionSpec as P

EPS = 1e-05
BF = jnp.bfloat16
F32 = jnp.float32
MESH = pl.DeviceIdType.MESH


def matrix_product(left, right):
    return jnp.dot(left, right, preferred_element_type=F32)


def matmul_tn(left, right):
    return lax.dot_general(left, right, (((0,), (0,)), ((), ())), preferred_element_type=F32)


def matrix_product_transposed(left, right):
    return lax.dot_general(left, right, (((1,), (1,)), ((), ())), preferred_element_type=F32)


def rope_tables(length, width):
    half = width // 2
    positions = jnp.arange(length).astype(F32)
    rates = jnp.exp(-math.log(10000.0) * jnp.arange(half).astype(F32) / half)
    angles = positions[:, None] * rates[None, :]
    cosine, sine = jnp.cos(angles), jnp.sin(angles)
    return jnp.concatenate([cosine, cosine], 1), jnp.concatenate([-sine, sine], 1)


def _dot(left, right, dims=((1,), (0,))):
    return lax.dot_general(left, right, (dims, ((), ())), preferred_element_type=F32)


def _split(value):
    high = value.astype(BF)
    return high, (value - high.astype(F32)).astype(BF)


def _head_weights(q, k, cosine, sine, allowed):
    width = q.shape[1]
    q = q * cosine + pltpu.roll(q, width // 2, 1) * sine
    k = k * cosine + pltpu.roll(k, width // 2, 1) * sine
    q_high, q_low = _split(q)
    k_high, k_low = _split(k)
    rows = ((1,), (1,))
    scores = _dot(q_high, k_high, rows) + _dot(q_high, k_low, rows) + _dot(q_low, k_high, rows)
    weights = jnp.where(allowed, jnp.exp(scores / math.sqrt(width)), 0.0)
    return weights / jnp.sum(weights, -1, keepdims=True), q_high, k_high


def _allowed(seg_col, seg_row):
    length = seg_col.shape[0]
    first = lax.broadcasted_iota(jnp.int32, (length, length), 0)
    second = lax.broadcasted_iota(jnp.int32, (length, length), 1)
    return (first >= second) & (seg_col[...] == seg_row[...])


def attention_forward(qkv, cosine, sine, seg_col, seg_row, o):
    width = cosine.shape[1]
    allowed = _allowed(seg_col, seg_row)
    for head in range(qkv.shape[2] // width):
        part = pl.ds(head * width, width)
        weights, _, _ = _head_weights(
            qkv[0, :, part], qkv[1, :, part], cosine[...], sine[...], allowed
        )
        o[:, part] = _dot(weights.astype(BF), qkv[2, :, part].astype(BF)).astype(BF)


def attention_backward(qkv, cosine, sine, seg_col, seg_row, grad, d_qkv):
    width = cosine.shape[1]
    allowed = _allowed(seg_col, seg_row)
    factor = 1.0 / math.sqrt(width)
    for head in range(qkv.shape[2] // width):
        part = pl.ds(head * width, width)
        weights, q_turned, k_turned = _head_weights(
            qkv[0, :, part], qkv[1, :, part], cosine[...], sine[...], allowed
        )
        grad_b = grad[:, part].astype(BF)
        d_weights = _dot(grad_b, qkv[2, :, part].astype(BF), ((1,), (1,)))
        inner = jnp.sum(d_weights * weights, -1, keepdims=True)
        d_scores = (weights * (d_weights - inner) * factor).astype(BF)
        d_turned = (
            _dot(d_scores, k_turned),
            _dot(d_scores, q_turned, ((0,), (0,))),
        )
        for i in range(2):
            d = d_turned[i]
            d = d * cosine[...] + pltpu.roll(d * sine[...], width // 2, 1)
            d_qkv[i, :, part] = d.astype(BF)
        d_qkv[2, :, part] = _dot(weights.astype(BF), grad_b, ((0,), (0,))).astype(BF)


def local_call(kernel, out_shape, *operands):
    vmem = pl.BlockSpec(memory_space=pltpu.VMEM)
    return pl.pallas_call(
        kernel,
        out_shape=out_shape,
        in_specs=[vmem] * len(operands),
        out_specs=jax.tree.map(lambda _: vmem, out_shape),
        name=kernel.__name__,
    )(*operands)


def conv_causal(signal, kernel, docs):
    total = signal * kernel[0]
    for offset in range(1, kernel.shape[0]):
        shifted = jnp.concatenate(
            [jnp.zeros((offset, signal.shape[1]), signal.dtype), signal[:-offset]], 0
        )
        shifted_docs = jnp.concatenate([jnp.full((offset,), -1, jnp.int32), docs[:-offset]], 0)
        same = (shifted_docs == docs).astype(signal.dtype)[:, None]
        total = total + shifted * kernel[offset] * same
    return total


def bc_activate(bc_pre, kernel, docs):
    return jax.nn.silu(conv_causal(bc_pre, kernel, docs))


def _decay(cum, cum_rows, head, allowed):
    gaps = cum[:, head : head + 1] - cum_rows[head : head + 1, :]
    return jnp.where(allowed, jnp.exp(jnp.where(allowed, gaps, 0.0)), 0.0)


def _thirds(value):
    high, rest = _split(value)
    rest = value - high.astype(F32)
    middle, low = _split(rest)
    return high, middle, low


def _triangle(length):
    first = lax.broadcasted_iota(jnp.int32, (length, length), 0)
    second = lax.broadcasted_iota(jnp.int32, (length, length), 1)
    return (first >= second).astype(F32).astype(BF)


def _running_sums(rate):
    lower = _triangle(rate.shape[0])
    parts = _thirds(rate)
    columns = sum(_dot(lower, part) for part in parts)
    rows = sum(_dot(part, lower, ((0,), (1,))) for part in parts)
    return columns, rows


def _intersection(bc):
    state = bc.shape[1] // 2
    b_high, b_low = _split(bc[:, :state])
    c_high, c_low = _split(bc[:, state:])
    rows = ((1,), (1,))
    total = _dot(c_high, b_high, rows) + _dot(c_high, b_low, rows) + _dot(c_low, b_high, rows)
    return total, b_high, c_high


def mixing_forward(bc, rate, weighted, doc_col, doc_row, o):
    heads = rate.shape[1]
    cum, cum_rows = _running_sums(rate[...])
    width = weighted.shape[1] // heads
    allowed = _allowed(doc_col, doc_row)
    intersection, _, _ = _intersection(bc[...])
    results = []
    for head in range(heads):
        mixing = _decay(cum, cum_rows, head, allowed) * intersection
        part = weighted[:, head * width : (head + 1) * width]
        results.append(_dot(mixing.astype(BF), part.astype(BF)))
    o[...] = jnp.concatenate(results, 1)


def mixing_backward(
    bc, rate, weighted, doc_col, doc_row, grad, d_bc, d_rate, d_weighted
):
    heads = rate.shape[1]
    cum, cum_rows = _running_sums(rate[...])
    lower = _triangle(rate.shape[0])
    width = weighted.shape[1] // heads
    allowed = _allowed(doc_col, doc_row)
    intersection, b, c = _intersection(bc[...])
    d_intersection = jnp.zeros_like(intersection)
    d_parts, ahead, behind = [], [], []
    for head in range(heads):
        decay = _decay(cum, cum_rows, head, allowed)
        mixing = decay * intersection
        part = weighted[:, head * width : (head + 1) * width].astype(BF)
        grad_part = grad[:, head * width : (head + 1) * width].astype(BF)
        d_parts.append(_dot(mixing.astype(BF), grad_part, ((0,), (0,))))
        d_mixing = _dot(grad_part, part, ((1,), (1,)))
        d_intersection = d_intersection + d_mixing * decay
        d_gaps = d_mixing * mixing
        ahead.append(jnp.sum(d_gaps, 1, keepdims=True))
        behind.append(jnp.sum(d_gaps, 0, keepdims=True))
    d_weighted[...] = jnp.concatenate(d_parts, 1)
    columns = sum(
        _dot(lower, part, ((0,), (0,))) for part in _thirds(jnp.concatenate(ahead, 1))
    )
    rows = sum(
        _dot(lower, part, ((0,), (1,))) for part in _thirds(jnp.concatenate(behind, 0))
    )
    d_rate[...] = columns - rows
    d_b = d_intersection.astype(BF)
    d_bc[...] = jnp.concatenate([_dot(d_b, c, ((0,), (0,))), _dot(d_b, b)], 1)


@jax.custom_vjp
def mixing_sum(bc, rate, weighted, doc_col, doc_row):
    shape = jax.ShapeDtypeStruct(weighted.shape, F32)
    return local_call(mixing_forward, shape, bc, rate, weighted, doc_col, doc_row)


def mixing_sum_forward(*operands):
    return mixing_sum(*operands), operands


def mixing_sum_backward(operands, grad):
    shapes = [jax.ShapeDtypeStruct(operand.shape, F32) for operand in operands[:3]]
    d_bc, d_rate, d_weighted = local_call(mixing_backward, shapes, *operands, grad)
    return d_bc, d_rate, d_weighted, None, None


mixing_sum.defvjp(mixing_sum_forward, mixing_sum_backward)


def mixer_core(
    x_pre,
    gate_z,
    step_raw,
    bc_conv,
    conv_kernel,
    step_offset_bias,
    log_decay_rates,
    head_skip_term,
    docs,
):
    length = x_pre.shape[0]
    heads = step_raw.shape[1]
    head_dim = x_pre.shape[1] // heads
    inner = jax.nn.silu(conv_causal(x_pre, conv_kernel, docs)).reshape(length, heads, head_dim)
    step = jax.nn.softplus(step_raw + step_offset_bias)
    rate = -jnp.exp(log_decay_rates) * step
    weighted = (inner * step[:, :, None]).reshape(length, -1)
    outputs = mixing_sum(
        bc_conv, rate, weighted, docs.reshape(length, 1), docs.reshape(1, length)
    ).reshape(inner.shape)
    outputs = outputs + head_skip_term[None, :, None] * inner
    return outputs.reshape(length, heads * head_dim) * jax.nn.silu(gate_z)


def gelu_product(gate_preact, up_preact):
    return jax.nn.gelu(gate_preact, approximate=True) * up_preact


def _window(index, size):
    return pl.ds(pl.multiple_of(index * size, size), size)


def _add_rows(rows, write):
    chunk = 64 if rows % 64 == 0 else rows
    if rows == chunk:
        write(pl.ds(0, rows))
        return

    def step(i, carry):
        write(pl.ds(pl.multiple_of(i * chunk, chunk), chunk))
        return carry

    lax.fori_loop(0, rows // chunk, step, 0)


def _remote(src, dst, send, recv, device):
    copy = pltpu.make_async_remote_copy(
        src_ref=src,
        dst_ref=dst,
        send_sem=send,
        recv_sem=recv,
        device_id=device,
        device_id_type=MESH,
    )
    copy.start()
    return copy


class Env:
    def __init__(self, n, replicas):
        self.n = n
        self.replicas = replicas
        self.dp = lax.axis_index("dp")
        self.col = lax.axis_index("col")
        self.row = lax.axis_index("row")
        self.sibling = {"row": 1 - self.row}

    def peer(self, k):
        return {"col": lax.rem(self.col + k, self.n)}

    def replica(self, k):
        return {"dp": lax.rem(self.dp + k, self.replicas)}


class Relay:

    def __init__(self, env, where, send, recv, direction):
        self.env, self.where, self.direction = env, where, direction
        self.send, self.recv = send, recv
        self.base = 0 if direction > 0 else env.n - 1
        self.neighbour = {"col": jnp.clip(env.col + direction, 0, env.n - 1)}

    def copy(self, step, source):
        i = self.base + step
        return pltpu.make_async_remote_copy(
            src_ref=source,
            dst_ref=self.where(self.owner(step)),
            send_sem=self.send.at[i],
            recv_sem=self.recv.at[i],
            device_id=self.neighbour,
            device_id_type=MESH,
        )

    def owner(self, step):
        owner = self.env.col - self.direction * step
        return jnp.clip(owner, 0, self.env.n - 1)

    def place(self):
        return self.env.col if self.direction > 0 else self.env.n - 1 - self.env.col

    def sends(self, step):
        return (self.place() < self.env.n - 1) & (self.place() >= step)

    def receives(self, step):
        return self.place() > step

    def start(self, step, source):
        @pl.when(self.sends(step))
        def _():
            self.copy(step, source).start()

    def arrived(self, step, then=None):
        @pl.when(self.receives(step))
        def _():
            part = self.where(self.owner(step + 1))
            pltpu.make_async_remote_copy(
                src_ref=part,
                dst_ref=part,
                send_sem=self.send.at[self.base + step],
                recv_sem=self.recv.at[self.base + step],
                device_id=self.neighbour,
                device_id_type=MESH,
            ).wait_recv()
            if then is not None:
                then(part, self.base + step)

    def sent(self, step, source):
        @pl.when(self.sends(step))
        def _():
            self.copy(step, source).wait_send()


def run_gather(env, x, o, send, recv, local):
    width = x.shape[1]

    def where(owner):
        return o.at[:, _window(owner, width)]

    own = pltpu.make_async_copy(x, where(env.col), local.at[0])
    ways = [Relay(env, where, send, recv, d) for d in (1, -1)]
    for way in ways:
        way.start(0, x)
    own.start()
    yield
    for step in range(env.n - 1):
        for way in ways:
            way.arrived(step)
            if step < env.n - 2:
                way.start(step + 1, where(way.owner(step + 1)))
        yield
    own.wait()
    for step in range(env.n - 1):
        for way in ways:
            way.sent(step, x)


def run_gather2(env, x, o, send, recv, local, send2, recv2):
    width = x.shape[1]
    half = x.shape[0] // 2
    mine = _window(env.row, half)

    def where(owner):
        return o.at[mine, _window(owner, width)]

    source = x.at[mine, :]

    def across(part, i):
        return pltpu.make_async_remote_copy(
            src_ref=part,
            dst_ref=part,
            send_sem=send2.at[i],
            recv_sem=recv2.at[i],
            device_id=env.sibling,
            device_id_type=MESH,
        )

    def pass_on(part, i):
        across(part, i).start()

    own = pltpu.make_async_copy(x, o.at[:, _window(env.col, width)], local.at[0])
    ways = [Relay(env, where, send, recv, d) for d in (1, -1)]
    for way in ways:
        way.start(0, source)
    own.start()
    yield
    for step in range(env.n - 1):
        for way in ways:
            way.arrived(step, pass_on)
            if step < env.n - 2:
                way.start(step + 1, where(way.owner(step + 1)))
        yield
    own.wait()
    for step in range(env.n - 1):
        for way in ways:
            way.sent(step, source)

            @pl.when(way.receives(step))
            def _(way=way, step=step):
                part = where(way.owner(step + 1))
                across(part, way.base + step).wait()


def run_scatter(env, p, o, buffer, send, recv):
    rows, width = o.shape
    copies = [
        _remote(
            p.at[:, _window(lax.rem(env.col + k, env.n), width)],
            buffer.at[k - 1],
            send.at[k - 1],
            recv.at[k - 1],
            env.peer(k),
        )
        for k in range(1, env.n)
    ]
    yield
    for copy in copies:
        copy.wait()

    def write(part):
        total = p[part, _window(env.col, width)].astype(F32)
        for k in range(env.n - 1):
            total = total + buffer[k, part, :].astype(F32)
        o[part, :] = total

    _add_rows(rows, write)


def run_scatter2(env, p, o, buffer, send, recv, send2, recv2):
    rows, width = p.shape[0], o.shape[1]
    size = rows // 2
    copies = []
    for c in range(2):
        for k in range(1, env.n):
            i = c * (env.n - 1) + k - 1
            part = pl.ds(c * size, size)
            copies.append(
                _remote(
                    p.at[part, _window(lax.rem(env.col + k, env.n), width)],
                    buffer.at[k - 1, part, :],
                    send.at[i],
                    recv.at[i],
                    env.peer(k),
                )
            )
    yield
    first = env.row * rows
    onward = []
    for c in range(2):
        for k in range(1, env.n):
            copies[c * (env.n - 1) + k - 1].wait()

        def write(part, c=c):
            source = pl.ds(pl.multiple_of(c * size + part.start, 16), part.size)
            total = p[source, _window(env.col, width)].astype(F32)
            for k in range(env.n - 1):
                total = total + buffer[k, source, :].astype(F32)
            target = pl.ds(pl.multiple_of(first + c * size + part.start, 8), part.size)
            o[target, :] = total

        _add_rows(size, write)
        half = o.at[_window(env.row * 2 + c, size), :]
        onward.append(_remote(half, half, send2.at[c], recv2.at[c], env.sibling))
    yield
    for copy in onward:
        copy.wait()


def run_reduce(env, p, o, pairs, sums, buffer, send, recv, send2, recv2, send3, recv3):
    rows, width = o.shape
    half = rows // 2
    size = half // 2
    other = _window(1 - env.row, half)
    order = [(k + 1) % env.n for k in range(env.n)]
    first = []
    for i, k in enumerate(order):
        piece = _window(lax.rem(env.col + k, env.n), width)
        first.append(
            _remote(p.at[other, piece], pairs.at[i], send.at[i], recv.at[i], env.sibling)
        )
    yield
    start = env.row * half
    copies = {}
    for i, k in enumerate(order):
        first[i].wait()
        piece = _window(lax.rem(env.col + k, env.n), width)

        def write(part, i=i, piece=piece):
            source = pl.ds(pl.multiple_of(start + part.start, 16), part.size)
            total = p[source, piece].astype(F32) + pairs[i, part, :].astype(F32)
            sums[i, part, :] = total.astype(sums.dtype)

        _add_rows(half, write)
        if k:
            for c in range(2):
                part = pl.ds(c * size, size)
                j = 2 * i + c
                copies[j] = _remote(
                    sums.at[i, part, :],
                    buffer.at[i, part, :],
                    send2.at[j],
                    recv2.at[j],
                    env.peer(k),
                )
    yield
    onward = []
    for c in range(2):
        for i in range(env.n - 1):
            copies[2 * i + c].wait()

        def finish(part, c=c):
            source = pl.ds(pl.multiple_of(c * size + part.start, 16), part.size)
            total = sums[env.n - 1, source, :].astype(F32)
            for k in range(env.n - 1):
                total = total + buffer[k, source, :].astype(F32)
            target = pl.ds(pl.multiple_of(start + c * size + part.start, 8), part.size)
            o[target, :] = total

        _add_rows(size, finish)
        part = o.at[_window(env.row * 2 + c, size), :]
        onward.append(_remote(part, part, send3.at[c], recv3.at[c], env.sibling))
    yield
    for copy in onward:
        copy.wait()


def run_a2a(env, x, o, send, recv, local):
    for _ in range(env.n - 2):
        yield
    width = o.shape[3]
    copies = [
        _remote(
            x.at[:, :, _window(lax.rem(env.col + k, env.n), width)],
            o.at[:, env.col],
            send.at[k - 1],
            recv.at[k - 1],
            env.peer(k),
        )
        for k in range(1, env.n)
    ]
    own = pltpu.make_async_copy(
        x.at[:, :, _window(env.col, width)], o.at[:, env.col], local.at[0]
    )
    own.start()
    yield
    own.wait()
    for copy in copies:
        copy.wait()


def run_a2a_back(delay, env, x, o, send, recv, local):
    for _ in range(delay):
        yield
    here = o.at[:, :, _window(env.col, x.shape[3])]
    copies = [
        _remote(
            x.at[:, lax.rem(env.col + k, env.n)],
            here,
            send.at[k - 1],
            recv.at[k - 1],
            env.peer(k),
        )
        for k in range(1, env.n)
    ]
    own = pltpu.make_async_copy(x.at[:, env.col], here, local.at[0])
    own.start()
    yield
    own.wait()
    for copy in copies:
        copy.wait()


def run_dpscatter(env, x, o, buffer, send, recv):
    groups, rows, _ = o.shape
    copies = [
        _remote(
            x.at[:, _window(lax.rem(env.dp + k, env.replicas), rows), :],
            buffer.at[k - 1],
            send.at[k - 1],
            recv.at[k - 1],
            env.replica(k),
        )
        for k in range(1, env.replicas)
    ]
    yield
    for copy in copies:
        copy.wait()
    start = env.dp * rows
    chunk = 64 if rows % 64 == 0 else rows
    steps = rows // chunk

    def step(i, carry):
        group = i // steps
        first = (i % steps) * chunk
        source = pl.ds(pl.multiple_of(start + first, 16), chunk)
        part = pl.ds(pl.multiple_of(first, 16), chunk)
        total = x[group, source, :].astype(F32)
        for k in range(env.replicas - 1):
            total = total + buffer[k, group, part, :].astype(F32)
        o[group, part, :] = total.astype(o.dtype)
        return carry

    lax.fori_loop(0, groups * steps, step, 0)


def run_dpgather(env, x, o, send, recv, local):
    here = o.at[:, _window(env.dp, x.shape[1]), :]
    copies = [
        _remote(x, here, send.at[k - 1], recv.at[k - 1], env.replica(k))
        for k in range(1, env.replicas)
    ]
    own = pltpu.make_async_copy(x, here, local.at[0])
    own.start()
    yield
    own.wait()
    for copy in copies:
        copy.wait()


def run_dpsum(env, s, o, buffer, send, recv, local):
    copies = [
        _remote(s, buffer.at[env.dp], send.at[k - 1], recv.at[k - 1], env.replica(k))
        for k in range(1, env.replicas)
    ]
    own = pltpu.make_async_copy(s, buffer.at[env.dp], local.at[0])
    own.start()
    yield
    own.wait()
    for copy in copies:
        copy.wait()
    total = buffer[0]
    for i in range(1, env.replicas):
        total = total + buffer[i]
    o[...] = total


def run_rowsum(env, p, o, buffer, send, recv):
    copy = _remote(p, buffer, send.at[0], recv.at[0], env.sibling)
    yield
    copy.wait()

    def write(part):
        o[part, :] = p[part, :].astype(F32) + buffer[part, :].astype(F32)

    _add_rows(p.shape[0], write)


def run_sum(env, s, o, buffer, send, recv, local):
    both = buffer.shape[0] > env.n
    mine = env.row * env.n + env.col if both else env.col
    copies = []
    for r in range(2 if both else 1):
        for k in range(env.n):
            if r == 0 and k == 0:
                continue
            device = dict(env.peer(k)) if k else {}
            if r:
                device["row"] = 1 - env.row
            index = r * env.n + k - 1
            copies.append(_remote(s, buffer.at[mine], send.at[index], recv.at[index], device))
    own = pltpu.make_async_copy(s, buffer.at[mine], local.at[0])
    own.start()
    yield
    own.wait()
    for copy in copies:
        copy.wait()
    total = buffer[0]
    for i in range(1, buffer.shape[0]):
        total = total + buffer[i]
    o[...] = total


def plan(kind, x, n, replicas):
    dma = pltpu.SemaphoreType.DMA
    shape = x.shape
    three = dma((n - 1,))
    one, two = dma((1,)), dma((2,))
    twice = dma((2 * (n - 1),))
    if kind == "gather":
        return run_gather, (shape[0], n * shape[1]), x.dtype, [twice, twice, one]
    if kind == "gather2":
        scratch = [twice, twice, one, twice, twice]
        return run_gather2, (shape[0], n * shape[1]), x.dtype, scratch
    if kind == "scatter":
        out = (shape[0], shape[1] // n)
        return run_scatter, out, F32, [pltpu.VMEM((n - 1,) + out, x.dtype), three, three]
    if kind == "scatter2":
        part = (shape[0], shape[1] // n)
        out = (2 * shape[0], shape[1] // n)
        scratch = [pltpu.VMEM((n - 1,) + part, x.dtype), twice, twice, two, two]
        return run_scatter2, out, F32, scratch
    if kind == "reduce":
        out = (shape[0], shape[1] // n)
        part = (shape[0] // 2, shape[1] // n)
        four = dma((n,))
        scratch = [
            pltpu.VMEM((n,) + part, x.dtype),
            pltpu.VMEM((n,) + part, x.dtype),
            pltpu.VMEM((n - 1,) + part, x.dtype),
            four,
            four,
            twice,
            twice,
            two,
            two,
        ]
        return run_reduce, out, F32, scratch
    if kind == "a2a":
        return run_a2a, (shape[0], n, shape[1], shape[2] // n), x.dtype, [three, three, one]
    if kind.startswith("a2a_back"):
        delay = {"a2a_back": 0, "a2a_back1": 1, "a2a_back2": n - 2}[kind]
        run = functools.partial(run_a2a_back, delay)
        return run, (shape[0], shape[2], n * shape[3]), x.dtype, [three, three, one]
    if kind.startswith("dp"):
        others = dma((replicas - 1,))
        if kind == "dpscatter":
            out = (shape[0], shape[1] // replicas, shape[2])
            return run_dpscatter, out, x.dtype, [
                pltpu.VMEM((replicas - 1,) + out, x.dtype),
                others,
                others,
            ]
        if kind == "dpgather":
            out = (shape[0], shape[1] * replicas, shape[2])
            return run_dpgather, out, x.dtype, [others, others, one]
        scratch = [pltpu.VMEM((replicas,) + shape, x.dtype), others, others, one]
        return run_dpsum, shape, F32, scratch
    if kind == "rowsum":
        return run_rowsum, shape, F32, [pltpu.VMEM(shape, x.dtype), one, one]
    members = n if kind == "colsum" else 2 * n
    many = dma((members - 1,))
    return run_sum, shape, F32, [pltpu.VMEM((members,) + shape, x.dtype), many, many, one]


def exchange(ident, items, micros):
    n = lax.axis_size("col")
    replicas = lax.axis_size("dp")
    plans = [plan(kind, x, n, replicas) for kind, x in items]
    kinds = {kind for kind, _ in items}
    count = len(items)
    use_all = "allsum" in kinds
    use_dp = any(kind.startswith("dp") for kind in kinds)
    use_col = use_all or any(kind != "rowsum" and not kind.startswith("dp") for kind in kinds)
    use_row = use_all or bool(kinds & {"rowsum", "gather2", "scatter2", "reduce"})

    def kernel(*refs):
        env = Env(n, replicas)
        barrier = pltpu.get_barrier_semaphore()
        targets = []
        if use_col:
            targets += [env.peer(k) for k in range(1, n)]
        if use_row:
            targets.append(env.sibling)
        if use_all:
            targets += [{**env.peer(k), **env.sibling} for k in range(1, n)]
        if use_dp:
            targets += [env.replica(k) for k in range(1, replicas)]
        for target in targets:
            pl.semaphore_signal(barrier, inc=1, device_id=target, device_id_type=MESH)
        pl.semaphore_wait(barrier, len(targets))
        position = 2 * count
        running = []
        for i in range(count):
            size = len(plans[i][3])
            scratch = refs[position : position + size]
            position += size
            running.append(plans[i][0](env, refs[i], refs[count + i], *scratch))
        while running:
            alive = []
            for item in running:
                try:
                    next(item)
                except StopIteration:
                    continue
                alive.append(item)
            running = alive

    vmem = pl.BlockSpec(memory_space=pltpu.VMEM)
    return pl.pallas_call(
        kernel,
        out_shape=[jax.ShapeDtypeStruct(p[1], p[2]) for p in plans],
        in_specs=[vmem] * count,
        out_specs=[vmem] * count,
        scratch_shapes=[s for p in plans for s in p[3]],
        compiler_params=pltpu.CompilerParams(collective_id=ident, has_side_effects=True),
        cost_estimate=pl.CostEstimate(
            flops=0, bytes_accessed=int(micros * 3000000), transcendentals=0
        ),
        name="exchange_%d" % ident,
    )(*[x for _, x in items])


def pack_rows(*vectors):
    return jnp.concatenate([v.reshape(-1, 128) for v in vectors], 0)


def unpack_rows(packed, count):
    return [part.reshape(-1) for part in jnp.split(packed, count, 0)]


def body(
    hidden_state_input,
    initial_token_embedding,
    document_numbers,
    document_start_flags,
    attention_norm_gain,
    query_key_value_matrix,
    attention_out_matrix,
    perceptron_norm_gain,
    gate_up_matrix,
    adapter_down,
    adapter_up,
    down_matrix,
    projection_matrix,
    mixer_norm_gain,
    gate_in_matrix,
    state_in_matrix,
    mixer_input_kernel,
    state_conv_kernel,
    step_offset_bias,
    log_decay_rates,
    head_skip_term,
    gated_norm_gain,
    mixer_out_matrix,
    output_gradient,
):
    n = lax.axis_size("col")
    replicas = lax.axis_size("dp")
    dp, row, col = lax.axis_index("dp"), lax.axis_index("row"), lax.axis_index("col")
    length, width = hidden_state_input.shape
    local_width = 2 * width
    model_width = n * width
    concat_width = n * local_width
    inner_width = gated_norm_gain.shape[0] * 2 * n

    def my_rows(weight):
        share = weight.shape[2] // replicas
        part = lax.dynamic_slice_in_dim(weight, dp * share, share, 2)
        return part.reshape(weight.shape[0], -1, weight.shape[3])

    def spread(pieces, inner):
        outer, own = pieces.shape[0], pieces.shape[3]
        shaped = pieces.reshape(outer, n, inner, -1, own)
        full = lax.all_gather(shaped, "dp", axis=3, tiled=True)
        return full.reshape(outer, -1, own)

    def after(value, *others):
        return lax.optimization_barrier((value,) + others)[0]

    attn_gain = attention_norm_gain.reshape(local_width)
    mlp_gain = perceptron_norm_gain.reshape(local_width)
    attn_out_flat = attention_out_matrix.reshape(attention_out_matrix.shape[0], local_width)
    down_flat = down_matrix.reshape(down_matrix.shape[0], local_width)
    proj_flat = projection_matrix.reshape(local_width, projection_matrix.shape[2])
    adapter_up_broad = adapter_up.astype(F32)
    state_width = state_in_matrix.shape[1]
    state_pad = jnp.pad(state_in_matrix, ((0, 0), (0, -state_width % 128)))

    (qkv_pieces,) = exchange(0, [("a2a", my_rows(query_key_value_matrix))], 20)
    qkv_t = spread(qkv_pieces, 2)

    concat = (
        jnp.stack([hidden_state_input, initial_token_embedding], 1)
        .astype(F32)
        .reshape(length, local_width)
    )
    x_one, sum_one, gate_up_pieces, gate_in_pieces, adapter_down_full, state_full = exchange(
        1,
        [
            ("gather2", after((concat * attn_gain).astype(BF), qkv_pieces)),
            ("colsum", pack_rows(jnp.sum(concat * concat, 1))),
            ("a2a", my_rows(gate_up_matrix)),
            ("a2a", my_rows(gate_in_matrix[:, None])),
            ("gather2", adapter_down.reshape(local_width, -1)),
            ("gather2", state_pad),
        ],
        60,
    )

    gate_up_t = spread(after(gate_up_pieces, qkv_t), 2)
    gate_in_t = spread(after(gate_in_pieces, gate_up_t), 1)

    def stacked(gathered, lanes):
        rows = gathered.shape[0]
        return gathered.reshape(rows, n, lanes).transpose(1, 0, 2).reshape(n * rows, lanes)

    down_full = stacked(adapter_down_full, adapter_down.shape[2])
    state_in_full = stacked(state_full, state_pad.shape[1])[:, :state_width]

    d_normed_four = lax.psum_scatter(
        matrix_product_transposed(output_gradient, mixer_out_matrix).astype(BF)[None],
        "col",
        scatter_dimension=2,
        tiled=True,
    )[0].astype(F32)

    scale_one = lax.rsqrt(sum_one.reshape(-1) / concat_width + EPS)[:, None]
    norm_one = concat * scale_one
    normed_one = (x_one.astype(F32) * scale_one).astype(BF)
    head_size = 128
    qkv_own = jnp.einsum("tk,iko->ito", normed_one, qkv_t, preferred_element_type=F32)
    shared_tables = (
        *rope_tables(length, head_size),
        document_numbers.reshape(length, 1),
        document_numbers.reshape(1, length),
    )
    attended = local_call(
        attention_forward,
        jax.ShapeDtypeStruct((length, qkv_own.shape[2]), BF),
        qkv_own,
        *shared_tables,
    )
    (heads_half,) = exchange(2, [("gather", attended)], 25)
    (attn_sum,) = exchange(
        3, [("rowsum", matrix_product(heads_half, attn_out_flat).astype(BF))], 5
    )
    attn_stream = concat + attn_sum
    x_two, sum_two = exchange(
        4,
        [
            ("gather2", (attn_stream * mlp_gain).astype(BF)),
            ("colsum", pack_rows(jnp.sum(attn_stream * attn_stream, 1))),
        ],
        25,
    )
    scale_two = lax.rsqrt(sum_two.reshape(-1) / concat_width + EPS)[:, None]
    norm_two = attn_stream * scale_two
    normed_two = (x_two.astype(F32) * scale_two).astype(BF)
    adapter_middle = matrix_product(normed_two, down_full)
    gate_up_local = jnp.einsum("tk,iko->ito", normed_two, gate_up_t, preferred_element_type=F32)
    gate_up_local = gate_up_local + jnp.einsum(
        "gb,sbm->sgm", adapter_middle, adapter_up_broad
    )
    hidden_own = gelu_product(gate_up_local[0], gate_up_local[1]).astype(BF)
    (hidden_half,) = exchange(5, [("gather", hidden_own)], 45)
    (mlp_sum,) = exchange(6, [("rowsum", matrix_product(hidden_half, down_flat).astype(BF))], 5)
    mixed_b = (attn_stream + mlp_sum).astype(BF)
    half_tokens = lax.dynamic_slice_in_dim(mixed_b, row * (length // 2), length // 2, 0)
    (proj_sum,) = exchange(7, [("scatter2", matrix_product(half_tokens, proj_flat).astype(BF))], 15)
    resid = hidden_state_input.astype(F32) + proj_sum
    x_three, sum_three = exchange(
        8,
        [
            ("gather2", (resid * mixer_norm_gain).astype(BF)),
            ("colsum", pack_rows(jnp.sum(resid * resid, 1))),
        ],
        15,
    )
    scale_three = lax.rsqrt(sum_three.reshape(-1) / model_width + EPS)[:, None]
    norm_three = resid * scale_three
    normed_three = (x_three.astype(F32) * scale_three).astype(BF)
    zx_own = jnp.einsum("tk,iko->ito", normed_three, gate_in_t, preferred_element_type=F32)
    bcdt = matrix_product(normed_three, state_in_full)
    state_cols = state_conv_kernel.shape[1]
    heads_own = step_offset_bias.shape[0]
    owner = row * n + col
    step_own = lax.dynamic_slice_in_dim(bcdt, state_cols + owner * heads_own, heads_own, 1)
    docs = jnp.cumsum(document_start_flags) - 1
    bc_conv, bc_back = jax.vjp(
        functools.partial(bc_activate, docs=docs), bcdt[:, :state_cols], state_conv_kernel
    )
    gated, core_back = jax.vjp(
        functools.partial(mixer_core, docs=docs),
        zx_own[1],
        zx_own[0],
        step_own,
        bc_conv,
        mixer_input_kernel,
        step_offset_bias,
        log_decay_rates,
        head_skip_term,
    )
    grad_hat = d_normed_four * gated_norm_gain
    (sums_four,) = exchange(
        9,
        [("allsum", pack_rows(jnp.sum(gated * gated, 1), jnp.sum(grad_hat * gated, 1)))],
        6,
    )
    square_four, cross_four = unpack_rows(sums_four, 2)
    scale_four = lax.rsqrt(square_four / inner_width + EPS)[:, None]
    norm_four = gated * scale_four
    inner_four = cross_four[:, None] * scale_four / inner_width
    d_gated = scale_four * (grad_hat - norm_four * inner_four)
    grad_gated_gain = jnp.sum(d_normed_four * norm_four, 0)
    normed_half = lax.all_gather(
        (norm_four * gated_norm_gain).astype(BF)[None], "col", axis=2, tiled=True
    )[0]

    (
        d_x_pre,
        d_gate_z,
        d_step_own,
        d_bc_part,
        grad_mixer_input_kernel,
        grad_step_offset_bias,
        grad_log_decay,
        grad_head_skip,
    ) = core_back(d_gated)
    step_slot = lax.dynamic_update_slice_in_dim(
        jnp.zeros((length, state_width - state_cols), F32), d_step_own, owner * heads_own, 1
    )
    d_bc_pre, grad_state_conv_kernel = bc_back(d_bc_part)
    d_bcdt_b = jnp.concatenate([d_bc_pre, step_slot], 1).astype(BF)
    d_zx_own = jnp.stack([d_gate_z, d_x_pre]).astype(BF)
    partial_three = jnp.einsum(
        "ito,iko->tk", d_zx_own, gate_in_t, preferred_element_type=F32
    ) + matrix_product_transposed(d_bcdt_b, state_in_full)
    cross_three = jnp.sum(d_zx_own.astype(F32) * zx_own, (0, 2)) + jnp.sum(
        d_bcdt_b.astype(F32) * bcdt, 1
    )
    grad_gate_in = jnp.einsum("tk,ito->iko", normed_three, d_zx_own, preferred_element_type=F32)

    def split_features(grad, inner):
        outer, own = grad.shape[0], grad.shape[2]
        return grad.astype(BF).reshape(outer, n, inner, -1, own)

    def grouped(grad, inner):
        groups = split_features(grad, inner)
        return groups.reshape((-1,) + groups.shape[3:])

    def ungrouped(share, outer):
        return share.reshape(outer, n, -1, share.shape[2])

    def share_of(grad, inner):
        share = lax.psum_scatter(
            split_features(grad, inner), "dp", scatter_dimension=3, tiled=True
        )
        return share.reshape(share.shape[0], n, -1, share.shape[4])

    def joined(back, inner):
        shaped = back.reshape(back.shape[0], inner, -1, back.shape[2])
        return lax.all_gather(shaped, "dp", axis=2, tiled=True)

    d_normed_three, inner_three, gate_in_share = exchange(
        10,
        [
            ("reduce", after(partial_three.astype(BF), normed_half)),
            ("allsum", pack_rows(cross_three)),
            ("dpscatter", grouped(grad_gate_in, 1)),
        ],
        25,
    )

    def norm_back(grad_in, inner, normal, scale, gain, count):
        mean = inner.reshape(-1)[:, None] / count
        return scale * (grad_in * gain - normal * mean), jnp.sum(grad_in * normal, 0)

    grad_state_in_part = matmul_tn(normed_three, d_bcdt_b)
    d_norm_three, grad_mixer_gain = norm_back(
        d_normed_three, inner_three, norm_three, scale_three, mixer_norm_gain, model_width
    )
    d_resid = output_gradient.astype(F32) + d_norm_three
    d_resid_full, conv_sum, gate_in_back = exchange(
        11,
        [
            ("gather2", d_resid.astype(BF)),
            ("allsum", grad_state_conv_kernel),
            ("a2a_back2", ungrouped(gate_in_share, 2)),
        ],
        28,
    )
    gate_in_wide = joined(gate_in_back, 1)
    grad_proj = matmul_tn(mixed_b, d_resid_full).astype(BF)
    d_mixed = matrix_product_transposed(d_resid_full, proj_flat)
    d_mixed_b = d_mixed.astype(BF)
    grad_down = matmul_tn(hidden_half, d_mixed_b).astype(BF)
    partial_hidden = matrix_product_transposed(d_mixed_b, down_flat).astype(BF)
    d_hidden_own, proj_share, down_share = exchange(
        12,
        [
            ("scatter", partial_hidden),
            ("dpscatter", grad_proj[None]),
            ("dpscatter", grad_down[None]),
        ],
        50,
    )
    act_back = jax.vjp(gelu_product, gate_up_local[0], gate_up_local[1])[1]
    grad_gate_up_local = jnp.stack(act_back(d_hidden_own))
    grad_adapter_up = jnp.einsum(
        "mc,ymv->ycv", adapter_middle, grad_gate_up_local
    )
    middle_part = jnp.einsum(
        "oaj,opj->ap", grad_gate_up_local, adapter_up_broad
    ).astype(BF)
    d_gate_up_b = grad_gate_up_local.astype(BF)
    partial_two = jnp.einsum(
        "ito,iko->tk", d_gate_up_b, gate_up_t, preferred_element_type=F32
    ) + matrix_product_transposed(middle_part, down_full)
    cross_two = jnp.sum(d_gate_up_b.astype(F32) * gate_up_local, (0, 2))
    grad_gate_up = jnp.einsum(
        "tk,ito->iko", normed_two, d_gate_up_b, preferred_element_type=F32
    ).astype(BF)
    gate_up_share = share_of(grad_gate_up, 2)
    d_normed_two, inner_two = exchange(
        13,
        [
            ("reduce", after(partial_two.astype(BF), grad_gate_up)),
            ("allsum", pack_rows(cross_two)),
        ],
        30,
    )
    grad_adapter_down_part = matmul_tn(normed_two, middle_part).astype(BF)

    def by_owner(part):
        lanes = part.shape[1] + -part.shape[1] % 128
        padded = jnp.pad(part, ((0, 0), (0, lanes - part.shape[1])))
        return padded.reshape(n, -1, lanes).transpose(1, 0, 2).reshape(-1, n * lanes)
    d_norm_two, grad_perceptron_gain = norm_back(
        d_normed_two, inner_two, norm_two, scale_two, mlp_gain, concat_width
    )
    d_attn = d_mixed + d_norm_two
    d_attn_b = d_attn.astype(BF)
    grad_attention_out = matmul_tn(heads_half, d_attn_b).astype(BF)
    grad_up_flat = grad_adapter_up.astype(BF).reshape(-1, grad_adapter_up.shape[2])
    grad_mixer_out = matmul_tn(after(normed_half, d_normed_two), output_gradient).astype(BF)
    (
        adapter_down_sum,
        state_in_sum,
        gate_up_back,
        out_share,
        attn_out_share,
        up_share,
        proj_full,
        down_full_grad,
        d_heads_own,
    ) = exchange(
        14,
        [
            ("reduce", by_owner(grad_adapter_down_part)),
            ("reduce", by_owner(grad_state_in_part.astype(BF))),
            ("a2a_back1", gate_up_share),
            ("dpscatter", grad_mixer_out[None]),
            ("dpscatter", grad_attention_out[None]),
            ("dpscatter", grad_up_flat[None]),
            ("dpgather", proj_share),
            ("dpgather", down_share),
            (
                "scatter",
                after(
                    matrix_product_transposed(d_attn_b, attn_out_flat).astype(BF),
                    gate_in_wide,
                ),
            ),
        ],
        50,
    )
    gate_up_wide = joined(gate_up_back, 2)
    d_qkv_b = local_call(
        attention_backward,
        jax.ShapeDtypeStruct(qkv_own.shape, BF),
        qkv_own,
        *shared_tables,
        d_heads_own,
    )
    partial_one = jnp.einsum("ito,iko->tk", d_qkv_b, qkv_t, preferred_element_type=F32)
    cross_one = jnp.sum(d_qkv_b.astype(F32) * qkv_own, (0, 2))
    grad_qkv = jnp.einsum("tk,ito->iko", normed_one, d_qkv_b, preferred_element_type=F32)
    (
        d_normed_one,
        inner_one,
        qkv_share,
        adapter_down_share,
        state_in_share,
        out_sum,
    ) = exchange(
        15,
        [
            ("reduce", partial_one.astype(BF)),
            ("allsum", pack_rows(cross_one)),
            ("dpscatter", grouped(grad_qkv, 2)),
            ("dpscatter", adapter_down_sum.astype(BF)[None]),
            ("dpscatter", state_in_sum.astype(BF)[None]),
            ("rowsum", matrix_product(after(normed_half, d_normed_two), mixer_out_matrix).astype(BF)),
        ],
        50,
    )
    d_norm_one, grad_attention_gain = norm_back(
        d_normed_one, inner_one, norm_one, scale_one, attn_gain, concat_width
    )
    d_concat = (d_attn + d_norm_one).reshape(length, 2, width)
    grad_hidden = d_resid + d_concat[:, 0]
    grad_embed = d_concat[:, 1]

    small = (
        grad_attention_gain,
        grad_perceptron_gain,
        grad_mixer_gain,
        grad_mixer_input_kernel,
        grad_step_offset_bias,
        grad_log_decay,
        grad_head_skip,
        grad_gated_gain,
        conv_sum,
    )
    flat = jnp.concatenate([value.reshape(-1) for value in small])
    packed = jnp.pad(flat, (0, -flat.size % 1024)).reshape(-1, 128)
    outer = query_key_value_matrix.shape[0]
    (
        qkv_back,
        out_full,
        attn_out_full,
        up_full,
        adapter_down_sum,
        state_in_sum,
        packed_sum,
    ) = exchange(
        16,
        [
            ("a2a_back", ungrouped(qkv_share, outer)),
            ("dpgather", out_share),
            ("dpgather", attn_out_share),
            ("dpgather", up_share),
            ("dpgather", adapter_down_share),
            ("dpgather", state_in_share),
            ("dpsum", packed),
        ],
        20,
    )
    grad_query_key_value = joined(after(qkv_back, gate_up_wide), 2)
    block_out = (resid + after(out_sum, qkv_back)).astype(BF)
    summed, position = [], 0
    for value in small:
        part = packed_sum.reshape(-1)[position : position + value.size]
        summed.append(part.reshape(value.shape))
        position += value.size
    (
        grad_attention_gain,
        grad_perceptron_gain,
        grad_mixer_gain,
        grad_mixer_input_kernel,
        grad_step_offset_bias,
        grad_log_decay,
        grad_head_skip,
        grad_gated_gain,
        grad_state_conv_kernel,
    ) = summed

    def widened(value, like):
        return after(value, qkv_back).astype(F32).reshape(like.shape)

    return (
        block_out,
        grad_hidden,
        grad_embed,
        grad_attention_gain.reshape(attention_norm_gain.shape),
        grad_query_key_value.astype(F32).reshape(query_key_value_matrix.shape),
        widened(attn_out_full, attention_out_matrix),
        grad_perceptron_gain.reshape(perceptron_norm_gain.shape),
        widened(gate_up_wide, gate_up_matrix),
        widened(adapter_down_sum, adapter_down),
        widened(up_full, adapter_up),
        widened(down_full_grad, down_matrix),
        widened(proj_full, projection_matrix),
        grad_mixer_gain,
        widened(gate_in_wide, gate_in_matrix),
        widened(state_in_sum[:, :, :state_width], state_in_matrix),
        grad_mixer_input_kernel,
        grad_state_conv_kernel,
        grad_step_offset_bias,
        grad_log_decay,
        grad_head_skip,
        grad_gated_gain,
        widened(out_full, mixer_out_matrix),
    )


def solution(mesh):
    tokens = P("dp", "col")
    spread = ("row", "col")
    return jax.shard_map(
        body,
        mesh=mesh,
        in_specs=(
            tokens,
            tokens,
            P("dp"),
            P("dp"),
            P(None, "col"),
            P(None, None, "col", "row"),
            P("row", None, "col"),
            P(None, "col"),
            P(None, None, "col", "row"),
            P(None, "col", None),
            P(None, None, spread),
            P("row", None, "col"),
            P(None, "col", None),
            P("col"),
            P(None, "col", "row"),
            P("col", None),
            P(None, spread),
            P(),
            P(spread),
            P(spread),
            P(spread),
            P(spread),
            P("row", "col"),
            tokens,
        ),
        out_specs=(
            tokens,
            tokens,
            tokens,
            P(None, "col"),
            P(None, None, "col", "row"),
            P("row", None, "col"),
            P(None, "col"),
            P(None, None, "col", "row"),
            P(None, "col", None),
            P(None, None, spread),
            P("row", None, "col"),
            P(None, "col", None),
            P("col"),
            P(None, "col", "row"),
            P("col", None),
            P(None, spread),
            P(),
            P(spread),
            P(spread),
            P(spread),
            P(spread),
            P("row", "col"),
        ),
        check_vma=False,
    )
```
